32 devices in a mesh: samp: 16 (over z, y, x), tile: 2 (over core).
Axes of the slice: x: 2, y: 2, z: 4, core: 2. Of those that a mesh axis runs over, the one named last changes fastest.
Arguments:
- traits: bfloat16 [16384, 1024], P('samp'), may hold values from -300 to 300
- covariates: bfloat16 [16384, 32], P('samp'), may hold values from -6 to 6
- genotypes: int32 [16384, 512], P('samp', 'tile'), may hold values from 0 to 2
- shuffles: int32 [6, 16384], P(None, 'samp'), may hold values from 0 to 16383, as said below
Outputs:
- observed: float32 [1024, 512], P('samp', 'tile')
- perm_max: float32 [6, 1024], P(None, 'samp')
The draws below stay inside these ranges and needn't reach their ends.
Inputs may be any that keep to these rules, and one draw needn't show every extreme that they name: Row p of shuffles maps each aligned block of 1024 samples one to one onto the same block's samples.
All inputs are finite; a program needn't handle non-finite values.
Results may differ from the reference program's by a relative error of at most 0.0045.
Values sent between devices are 32-bit elements; how exact they have to be, the bound alone decides.
A program may use at most 64 MiB of HBM per device.

```python
import math
import jax
import jax.numpy as jnp
from jax import lax

SAMP_DEV = 1024
E = 1024
C = 32
PERMS = 6
SAMPLES = 16384
VARIANTS = 512


def covariate_base(key):
    values = jax.random.normal(jax.random.fold_in(key, 11), (SAMPLES, C), jnp.float32)
    return jnp.clip(values, -6.0, 6.0)


def draw_covariates(key, part):
    return covariate_base(key).astype(jnp.bfloat16)


def draw_traits(key, part):
    base = covariate_base(key)
    key_load, key_mean, key_noise, key_cols = jax.random.split(jax.random.fold_in(key, 23), 4)
    loading = jax.random.normal(key_load, (C, E), jnp.float32) / math.sqrt(C)
    means = 2.0 * jnp.clip(jax.random.normal(key_mean, (E,), jnp.float32), -4.0, 4.0)
    col_scale = jnp.exp(jax.random.uniform(key_cols, (E,), jnp.float32, 0.0, math.log(10.0)))
    position = jnp.arange(SAMPLES, dtype=jnp.float32) / SAMPLES
    noise = jnp.clip(jax.random.normal(key_noise, (SAMPLES, E), jnp.float32), -5.0, 5.0)
    row_scale = 1.0 + 2.0 * position
    fitted = jnp.dot(base, loading, precision=lax.Precision.HIGHEST)
    values = (means[None, :] + fitted + noise) * row_scale[:, None] * col_scale[None, :]
    return jnp.clip(values, -300.0, 300.0).astype(jnp.bfloat16)


def draw_genotypes(key, part):
    key_freq, key_first, key_second = jax.random.split(jax.random.fold_in(key, 37), 3)
    freq = jax.random.randint(key_freq, (1, VARIANTS), 5, 96)
    first = (jax.random.randint(key_first, (SAMPLES, VARIANTS), 0, 100) < freq).astype(jnp.int32)
    second = (jax.random.randint(key_second, (SAMPLES, VARIANTS), 0, 100) < freq).astype(jnp.int32)
    return first + second


def draw_shuffles(key, part):
    blocks = SAMPLES // SAMP_DEV
    keys = jax.random.split(jax.random.fold_in(key, 41), PERMS * blocks)
    orders = jax.vmap(lambda one_key: jax.random.permutation(one_key, SAMP_DEV))(keys).astype(jnp.int32)
    offsets = jnp.arange(blocks, dtype=jnp.int32) * SAMP_DEV
    orders = orders.reshape(PERMS, blocks, SAMP_DEV) + offsets[None, :, None]
    return orders.reshape(PERMS, SAMPLES).astype(jnp.int32)


def setup_inputs(seed: int = 0) -> dict:
    key_of = jax.random.split(jax.random.key(seed), 5)
    return {
        "traits": draw_traits(jax.random.fold_in(key_of[4], 71), 0),
        "covariates": draw_covariates(jax.random.fold_in(key_of[4], 71), 0),
        "genotypes": draw_genotypes(jax.random.fold_in(key_of[4], 71), 0),
        "shuffles": draw_shuffles(jax.random.fold_in(key_of[4], 71), 0),
    }


epsilon = 1e-05

def cholesky_solve(factor, rhs):
    first = lax.linalg.triangular_solve(factor, rhs, left_side=True, lower=True)
    return lax.linalg.triangular_solve(factor, first, left_side=True, lower=True, transpose_a=True)

def reference(traits, covariates, genotypes, shuffles):
    ones = jnp.ones((covariates.shape[0], 1), jnp.bfloat16)
    design = jnp.concatenate([ones, covariates], axis=1)
    dosage = genotypes.astype(jnp.bfloat16)
    gram = jnp.dot(design.T.astype(jnp.float32), design.astype(jnp.float32), preferred_element_type=jnp.float32)
    xty = jnp.dot(design.T.astype(jnp.float32), traits.astype(jnp.float32), preferred_element_type=jnp.float32)
    xtg = jnp.dot(design.T.astype(jnp.float32), dosage.astype(jnp.float32), preferred_element_type=jnp.float32)
    factor = jnp.linalg.cholesky(gram)
    coef_traits = cholesky_solve(factor, xty).astype(jnp.bfloat16)
    coef_geno = cholesky_solve(factor, xtg).astype(jnp.bfloat16)
    resid_traits = traits.astype(jnp.float32) - jnp.dot(design.astype(jnp.float32), coef_traits.astype(jnp.float32), preferred_element_type=jnp.float32)
    resid_geno = dosage.astype(jnp.float32) - jnp.dot(design.astype(jnp.float32), coef_geno.astype(jnp.float32), preferred_element_type=jnp.float32)
    mean_traits = lax.optimization_barrier(jnp.sum(resid_traits * resid_traits, axis=0)) / SAMPLES
    mean_geno = lax.optimization_barrier(jnp.sum(resid_geno * resid_geno, axis=0)) / SAMPLES
    rt_rows = resid_traits.astype(jnp.bfloat16)
    rg_rows = resid_geno.astype(jnp.bfloat16)
    scale_traits = lax.rsqrt(mean_traits + epsilon)
    scale_geno = lax.rsqrt(mean_geno + epsilon)
    factor_z = math.sqrt(SAMPLES - C - 2) / SAMPLES

    def scores_of(trait_rows):
        cross = jnp.dot(trait_rows.T.astype(jnp.float32), rg_rows.astype(jnp.float32), preferred_element_type=jnp.float32)
        return cross * scale_traits[:, None] * scale_geno[None, :] * factor_z
    observed = scores_of(rt_rows)

    def one_perm(order):
        shuffled = jnp.take(rt_rows, order.astype(jnp.int32), axis=0)
        return lax.optimization_barrier(jnp.max(jnp.abs(scores_of(shuffled)), axis=1))
    perm_max = lax.map(one_perm, shuffles)
    return (observed, perm_max)
```

```python
import functools
import math

import jax
import jax.numpy as jnp
from jax import lax
from jax.experimental import pallas as pl
from jax.experimental.pallas import tpu as pltpu
from jax.sharding import PartitionSpec as P

MESH = pl.DeviceIdType.MESH
LANES = 128
F32, BF16 = jnp.float32, jnp.bfloat16
HIGHEST = lax.Precision.HIGHEST
epsilon = 1e-05


def parts_of(bits, own, width):
    cut, half = own - max(8, own // 32 * 8), width // 2
    low, high, rest = tuple(range(2)), tuple(range(2, bits)), tuple(range(3, bits))
    return (
        ((0, 1) + high, slice(0, cut), slice(0, half)),
        ((1, 0) + high, slice(0, cut), slice(half, width)),
        (high + low, slice(cut, own), slice(0, half)),
        ((2, 1, 0) + rest, slice(cut, own), slice(half, width)),
    )


def place_of(order, g):
    at = [(g >> bit) & 1 for bit in order]
    rest = 0
    for bit in at[1:]:
        rest = 2 * rest + bit
    return at[0], rest


def scan_kernel(
    groups, tiles, samples, used, areas, t_hbm, c_hbm, g_hbm, order_hbm, score_ref, peak_ref,
    t_ref, c_ref, g_ref, order_ref, load, design, parts, landed, mine, full, rhs, coef, rt, rg,
    moved, found, fix, gram_ref, notes, squares, column, peaks, sum_sems, sq_send, sq_recv,
    tile_send, tile_recv, send, recv, *bufs
):
    me = lax.axis_index("samp")
    my_tile = lax.axis_index("tile")
    turns, width, n_parts = found.shape[0], found.shape[2], len(areas)
    bits = len(areas[0][0])
    local, traits = t_ref.shape
    own = traits // groups
    share = traits // tiles
    quota = parts.shape[0] // groups

    def samp_peer(d):
        return {"samp": lax.rem(me + d, groups)}

    def tile_peer(d):
        return {"tile": lax.rem(my_tile + d, tiles)}

    barrier = pltpu.get_barrier_semaphore()
    for d in range(1, groups):
        pl.semaphore_signal(barrier, inc=1, device_id=samp_peer(d), device_id_type=MESH)
    for d in range(1, tiles):
        pl.semaphore_signal(barrier, inc=1, device_id=tile_peer(d), device_id_type=MESH)
    loads = [
        pltpu.make_async_copy(a, b, load.at[i])
        for i, (a, b) in enumerate(
            ((c_hbm, c_ref), (t_hbm, t_ref), (g_hbm, g_ref), (order_hbm, order_ref))
        )
    ]
    for copy in loads:
        copy.start()
    for copy in loads:
        copy.wait()

    lane = lax.broadcasted_iota(jnp.int32, (LANES - used + 1, local), 0)
    design_t = jnp.concatenate(
        [c_ref[...].astype(F32), jnp.where(lane == 0, 1.0, 0.0)], axis=0
    )
    design[...] = design_t.T.astype(BF16)
    design_t = design_t[: -(-used // 16) * 16].astype(BF16)
    n_t, n_g = share // LANES, width // LANES
    n_blocks = n_t + n_g + 1
    whole, rest = used // 8, used % 8
    strips = -(-used // 8)

    def spot(c, r):
        at = c * rest + r
        return n_blocks * whole + at // 8, at % 8

    for i in range(n_blocks * whole, parts.shape[0]):
        parts[i] = jnp.zeros((8, LANES), F32)
    dose = g_ref[...].astype(F32)
    first = 0
    for block in (
        t_ref[:, pl.ds(pl.multiple_of(my_tile * share, LANES), share)],
        dose.astype(BF16),
        design[...],
    ):
        block = jnp.dot(design_t, block, preferred_element_type=F32)
        for c in range(block.shape[1] // LANES):
            at = slice(LANES * c, LANES * c + LANES)
            for r in range(whole):
                parts[(first + c) * whole + r] = block[8 * r : 8 * r + 8, at]
            for r in range(rest):
                slot, row = spot(first + c, r)
                parts[slot, row : row + 1, :] = block[8 * whole + r : 8 * whole + r + 1, at]
        first += block.shape[1] // LANES

    def source(p, stage):
        return bufs[2 * p * bits + 2 * stage]

    def target(p, stage):
        return bufs[2 * p * bits + 2 * stage + 1]

    def side(p, stage):
        bit = areas[p][0][stage]
        return lax.rem(me // 2**bit, 2), 2**bit

    def copies(k, stage):
        out = []
        for p in range(n_parts):
            b, far = side(p, stage)
            out.append(
                pltpu.make_async_remote_copy(
                    src_ref=source(p, stage).at[k, 1 - b],
                    dst_ref=target(p, stage).at[k],
                    send_sem=send.at[k, p, stage],
                    recv_sem=recv.at[k, p, stage],
                    device_id={"samp": me + (1 - 2 * b) * far},
                    device_id_type=MESH,
                )
            )
        return out

    def begin(k, stage):
        for copy in copies(k, stage):
            copy.start()

    def collect(k, stage):
        for copy in copies(k, stage):
            copy.wait_recv()
        for p in range(n_parts):
            b, _ = side(p, stage)
            total = source(p, stage)[k, b] + target(p, stage)[k]
            if stage < bits - 1:
                source(p, stage + 1)[k] = total.reshape(source(p, stage + 1).shape[1:])
            else:
                found[k, areas[p][1], areas[p][2]] = total[0]

    def cross(k, right):
        batch = max(groups // 4, 1)
        for q in range(groups // batch):
            rows = batch * own
            block = jnp.dot(
                rt[q * rows : (q + 1) * rows, :], right, preferred_element_type=F32
            )
            for i in range(batch):
                for p in range(n_parts):
                    order, part_rows, part_lanes = areas[p]
                    lead, other = place_of(order, q * batch + i)
                    source(p, 0)[k, lead, other] = block[i * own : (i + 1) * own][
                        part_rows, part_lanes
                    ]

    step = min(256, local)
    for i in range(local // step):
        at = slice(i * step, (i + 1) * step)
        rt[:, at] = t_ref[at, :].T
    cross(0, (dose - 1.0).astype(BF16))
    pl.semaphore_wait(barrier, groups + tiles - 2)

    def sum_copy(d, source, target, stage):
        return pltpu.make_async_remote_copy(
            src_ref=source,
            dst_ref=target,
            send_sem=sum_sems.at[2 * stage, d - 1],
            recv_sem=sum_sems.at[2 * stage + 1, d - 1],
            device_id=samp_peer(d),
            device_id_type=MESH,
        )

    scattered = [
        sum_copy(d, parts.at[pl.ds(lax.rem(me + d, groups) * quota, quota)], landed.at[d - 1], 0)
        for d in range(1, groups)
    ]
    for copy in scattered:
        copy.start()
    begin(0, 0)
    total = parts[pl.ds(me * quota, quota)]
    for d in range(1, groups):
        scattered[d - 1].wait_recv()
        total = total + landed[d - 1]
    mine[...] = total
    full[my_tile, pl.ds(me * quota, quota)] = total
    gathered = [
        sum_copy(d, mine, full.at[my_tile, pl.ds(me * quota, quota)], 1)
        for d in range(1, groups)
    ]
    for copy in gathered:
        copy.start()
    rhs[...] = jnp.zeros(rhs.shape, F32)
    gram_ref[...] = jnp.zeros(gram_ref.shape, F32)
    coef[...] = jnp.zeros(coef.shape, BF16)
    collect(0, 0)
    begin(0, 1)
    for copy in gathered:
        copy.wait_recv()

    def spread_copy(d):
        return pltpu.make_async_remote_copy(
            src_ref=full.at[my_tile],
            dst_ref=full.at[my_tile],
            send_sem=tile_send.at[tiles - 1 + d - 1],
            recv_sem=tile_recv.at[tiles - 1 + d - 1],
            device_id=tile_peer(d),
            device_id_type=MESH,
        )

    spread = [spread_copy(d) for d in range(1, tiles)]
    for copy in spread:
        copy.start()
    collect(0, 1)
    begin(0, 2)

    half = LANES // 2
    last = n_blocks - 1
    for r in range(whole):
        gram_ref[8 * r : 8 * r + 8, :] = full[my_tile, last * whole + r]
    for r in range(rest):
        slot, row = spot(last, r)
        gram_ref[8 * whole + r : 8 * whole + r + 1, :] = full[my_tile, slot, row : row + 1, :]
    gram = gram_ref[: 8 * strips, :]
    sub = lax.broadcasted_iota(jnp.int32, gram.shape, 0)
    lane = lax.broadcasted_iota(jnp.int32, gram.shape, 1)
    gram = jnp.where(lane == sub + half, 1.0, gram)
    for j in range(used):
        row = gram[j : j + 1, :] * (1.0 / gram[j : j + 1, j : j + 1])
        gram = jnp.where(sub == j, row, gram - gram[:, j : j + 1] * row)
    inverse = jnp.where(lane >= half, gram, 0.0)
    for copy in spread:
        copy.wait_recv()
    for tile in range(tiles + 1):
        held = full.at[tile] if tile < tiles else full.at[my_tile]
        for c in range(n_t if tile < tiles else n_g):
            block = c + (0 if tile < tiles else n_t)
            at = LANES * (tile * n_t + c)
            for r in range(whole):
                rhs[half + 8 * r : half + 8 * r + 8, at : at + LANES] = held[block * whole + r]
            for r in range(rest):
                slot, row = spot(block, r)
                to = half + 8 * whole + r
                rhs[to : to + 1, at : at + LANES] = held[slot, row : row + 1, :]
    coef[: 8 * strips, :] = jnp.dot(
        inverse, rhs[...], precision=HIGHEST, preferred_element_type=F32
    ).astype(BF16)
    collect(0, 2)
    begin(0, 3)

    sq_t = jnp.zeros((1, traits), F32)
    sq_g = jnp.zeros((1, width), F32)
    for i in range(local // step):
        at = slice(i * step, (i + 1) * step)
        d = design[at, :]
        resid = t_ref[at, :].astype(F32) - jnp.dot(
            d, coef[:, :traits], preferred_element_type=F32
        )
        sq_t = sq_t + jnp.sum(resid * resid, axis=0, keepdims=True)
        rt[:, at] = resid.astype(BF16).T
        dose = g_ref[at, :].astype(F32)
        resid = dose - jnp.dot(d, coef[:, traits:], preferred_element_type=F32)
        sq_g = sq_g + jnp.sum(resid * resid, axis=0, keepdims=True)
        rg[at, :] = resid.astype(BF16)

    def note_squares():
        for j in range(groups):
            at = j * own // LANES * LANES
            notes[j, 0:1, :] = sq_t[:, at : at + LANES]
            for c in range(n_g):
                notes[j, 1 + c : 2 + c, :] = sq_g[:, c * LANES : (c + 1) * LANES]
            if n_g < 7:
                notes[j, 1 + n_g :, :] = jnp.zeros((7 - n_g, LANES), F32)

    def square_copy(d):
        return pltpu.make_async_remote_copy(
            src_ref=notes.at[lax.rem(me + d, groups)],
            dst_ref=squares.at[d],
            send_sem=sq_send.at[d - 1],
            recv_sem=sq_recv.at[d - 1],
            device_id=samp_peer(d),
            device_id_type=MESH,
        )

    note_squares()
    squares[0] = notes[me]

    def permute(k):
        order = order_ref[pl.ds(k - 1, 1), :] - me * local
        for i in range(local // step):
            row = lax.broadcasted_iota(jnp.int32, (step, local), 0) + i * step
            hot = jnp.where(row == order, 1.0, 0.0).astype(BF16)
            moved[i * step : (i + 1) * step, :] = jnp.dot(
                hot, rg[...], preferred_element_type=F32
            ).astype(BF16)

    lead = pl.multiple_of(me * own // LANES * LANES, LANES)
    shift = pl.multiple_of(lax.rem(me * own, LANES), 8)

    def correct():
        gram = gram_ref[...]
        lane = lax.broadcasted_iota(jnp.int32, gram.shape, 1)
        gram = jnp.where(lane < half, gram, 0.0)
        coef_g = coef[:, traits:].astype(F32)
        miss = rhs[half:, traits:] - jnp.dot(
            gram, coef_g, precision=HIGHEST, preferred_element_type=F32
        )
        sub = lax.broadcasted_iota(jnp.int32, (half, width), 0)
        fit = coef_g[:half] - jnp.where(sub == used - 1, 1.0, 0.0)
        left = jnp.concatenate(
            [rhs[half:, pl.ds(lead, LANES)], coef[:half, pl.ds(lead, LANES)].astype(F32)], axis=0
        )
        column[...] = left.T
        fix[...] = jnp.dot(
            column[pl.ds(shift, own), :],
            jnp.concatenate([fit, miss], axis=0),
            precision=HIGHEST,
            preferred_element_type=F32,
        )

    def turn(t, carry):
        @pl.when(t < turns)
        def _():
            permute(t)
            cross(t, moved[...])
            begin(t, 0)

        @pl.when(t == 1)
        def _():
            for d in range(1, groups):
                square_copy(d).start()
            correct()

        for stage in range(bits):
            k = t - 1 - stage

            @pl.when(jnp.logical_and(k >= (0 if stage > 2 else 1), k < turns))
            def _():
                collect(k, stage)
                if stage < bits - 1:
                    begin(k, stage + 1)

        return carry

    lax.fori_loop(1, turns + bits, turn, 0)

    total = squares[0]
    for d in range(1, groups):
        square_copy(d).wait_recv()
        total = total + squares[d]
    gain = lax.rsqrt(total / samples + epsilon)
    factor = math.sqrt(samples - used - 1) / samples
    gain_g = jnp.concatenate([gain[1 + c : 2 + c, :] for c in range(n_g)], axis=1)
    column[...] = jnp.broadcast_to(gain.T[:, :1] * factor, column.shape)
    gain_t = column[pl.ds(shift, own), :]
    gain_t = gain_t[:, :1]
    score_ref[...] = (found[0] - fix[...]) * gain_g * gain_t
    top = jnp.zeros((own, LANES), F32)
    pos = lax.broadcasted_iota(jnp.int32, top.shape, 1)
    for k in range(1, turns):
        peak = jnp.max(jnp.abs(found[k] * gain_g), axis=1, keepdims=True) * gain_t
        top = jnp.where(pos == k - 1, peak, top)
    peaks[0] = top
    crossed = [
        pltpu.make_async_remote_copy(
            src_ref=peaks.at[0],
            dst_ref=peaks.at[d],
            send_sem=tile_send.at[d - 1],
            recv_sem=tile_recv.at[d - 1],
            device_id=tile_peer(d),
            device_id_type=MESH,
        )
        for d in range(1, tiles)
    ]
    for copy in crossed:
        copy.start()
    for copy in scattered + gathered + spread:
        copy.wait_send()

    def finish(k, carry):
        for stage in range(bits):
            for copy in copies(k, stage):
                copy.wait_send()
        return carry

    lax.fori_loop(0, turns, finish, 0)
    for d in range(1, groups):
        square_copy(d).wait_send()
    for d in range(1, tiles):
        crossed[d - 1].wait()
        top = jnp.maximum(top, peaks[d])
    peak_ref[...] = top.T[: turns - 1]


def shards(traits, covariates, genotypes, shuffles):
    groups, tiles = lax.axis_size("samp"), lax.axis_size("tile")
    bits = groups.bit_length() - 1
    turns = shuffles.shape[0] + 1
    local, n_traits = traits.shape
    width = genotypes.shape[1]
    used = covariates.shape[1] + 1
    own = n_traits // groups
    areas = parts_of(bits, own, width)
    bufs = []
    for _, part_rows, part_lanes in areas:
        size = (part_rows.stop - part_rows.start, part_lanes.stop - part_lanes.start)
        for stage in range(bits):
            lot = 2 ** (bits - 1 - stage)
            bufs.append(pltpu.VMEM((turns, 2, lot) + size, F32))
            bufs.append(pltpu.VMEM((turns, lot) + size, F32))
    n_blocks = (n_traits // tiles + width) // LANES + 1
    slots = n_blocks * (used // 8) + -(-n_blocks * (used % 8) // 8)
    quota = -(-slots // groups)
    vmem = pl.BlockSpec(memory_space=pltpu.VMEM)
    sems = pltpu.SemaphoreType.DMA((turns, len(areas), bits))
    flat = pltpu.SemaphoreType.DMA((groups - 1,))
    pair = pltpu.SemaphoreType.DMA((max(2 * (tiles - 1), 1),))
    return pl.pallas_call(
        functools.partial(scan_kernel, groups, tiles, local * groups, used, areas),
        out_shape=(
            jax.ShapeDtypeStruct((own, width), F32),
            jax.ShapeDtypeStruct((turns - 1, own), F32),
        ),
        in_specs=[pl.BlockSpec(memory_space=pl.ANY)] * 4,
        out_specs=(vmem, vmem),
        scratch_shapes=[
            pltpu.VMEM((local, n_traits), BF16),
            pltpu.VMEM((used - 1, local), BF16),
            pltpu.VMEM((local, width), jnp.int32),
            pltpu.VMEM((turns - 1, local), jnp.int32),
            pltpu.SemaphoreType.DMA((4,)),
            pltpu.VMEM((local, LANES), BF16),
            pltpu.VMEM((quota * groups, 8, LANES), F32),
            pltpu.VMEM((groups - 1, quota, 8, LANES), F32),
            pltpu.VMEM((quota, 8, LANES), F32),
            pltpu.VMEM((tiles, quota * groups, 8, LANES), F32),
            pltpu.VMEM((LANES, n_traits + width), F32),
            pltpu.VMEM((LANES, n_traits + width), BF16),
            pltpu.VMEM((n_traits, local), BF16),
            pltpu.VMEM((local, width), BF16),
            pltpu.VMEM((local, width), BF16),
            pltpu.VMEM((turns, own, width), F32),
            pltpu.VMEM((own, width), F32),
            pltpu.VMEM((LANES // 2, LANES), F32),
            pltpu.VMEM((groups, 8, LANES), F32),
            pltpu.VMEM((groups, 8, LANES), F32),
            pltpu.VMEM((LANES, LANES), F32),
            pltpu.VMEM((tiles, own, LANES), F32),
            pltpu.SemaphoreType.DMA((4, groups - 1)),
            flat,
            flat,
            pair,
            pair,
            sems,
            sems,
            *bufs,
        ],
        compiler_params=pltpu.CompilerParams(
            collective_id=0, has_side_effects=True, vmem_limit_bytes=60 * 1024 * 1024
        ),
        name="scan",
    )(traits, covariates.T, genotypes, shuffles)


def solution(mesh):
    placed = (P("samp", None), P("samp", None), P("samp", "tile"), P(None, "samp"))
    return jax.shard_map(
        shards,
        mesh=mesh,
        in_specs=placed,
        out_specs=(P("samp", "tile"), P(None, "samp")),
        check_vma=False,
    )
```

```python
import functools
import math

import jax
import jax.numpy as jnp
from jax import lax
from jax.experimental import pallas as pl
from jax.experimental.pallas import tpu as pltpu
from jax.sharding import PartitionSpec as P

MESH = pl.DeviceIdType.MESH
LANES = 128
F32, BF16 = jnp.float32, jnp.bfloat16
HIGHEST = lax.Precision.HIGHEST
epsilon = 1e-05


def parts_of(bits, own, width):
    cut, half = own - max(8, own // 32 * 8), width // 2
    low, high, rest = tuple(range(2)), tuple(range(2, bits)), tuple(range(3, bits))
    mid = cut // 16 * 8
    return (
        ((0, 1) + high, slice(0, mid), slice(0, half)),
        ((1, 0) + high, slice(0, mid), slice(half, width)),
        ((0, 1) + high, slice(mid, cut), slice(0, half)),
        ((1, 0) + high, slice(mid, cut), slice(half, width)),
        (high + low, slice(cut, own), slice(0, half)),
        ((2, 1, 0) + rest, slice(cut, own), slice(half, width)),
    )


def place_of(order, g):
    at = [(g >> bit) & 1 for bit in order]
    rest = 0
    for bit in at[1:]:
        rest = 2 * rest + bit
    return at[0], rest


def scan_kernel(
    groups, tiles, samples, used, areas, t_hbm, c_hbm, g_hbm, order_hbm, score_ref, peak_ref,
    t_ref, c_ref, g_ref, order_ref, load, design, parts, landed, mine, full, rhs, coef, rt, rg,
    moved, found, fix, gram_ref, notes, squares, column, peaks, sum_sems, sq_send, sq_recv,
    tile_send, tile_recv, send, recv, *bufs
):
    me = lax.axis_index("samp")
    my_tile = lax.axis_index("tile")
    turns, width, n_parts = found.shape[0], found.shape[2], len(areas)
    bits = len(areas[0][0])
    local, traits = t_ref.shape
    own = traits // groups
    share = traits // tiles
    quota = parts.shape[0] // groups

    def samp_peer(d):
        return {"samp": lax.rem(me + d, groups)}

    def tile_peer(d):
        return {"tile": lax.rem(my_tile + d, tiles)}

    barrier = pltpu.get_barrier_semaphore()
    for d in range(1, groups):
        pl.semaphore_signal(barrier, inc=1, device_id=samp_peer(d), device_id_type=MESH)
    for d in range(1, tiles):
        pl.semaphore_signal(barrier, inc=1, device_id=tile_peer(d), device_id_type=MESH)
    loads = [
        pltpu.make_async_copy(a, b, load.at[i])
        for i, (a, b) in enumerate(
            ((c_hbm, c_ref), (t_hbm, t_ref), (g_hbm, g_ref), (order_hbm, order_ref))
        )
    ]
    for copy in loads:
        copy.start()
    for copy in loads:
        copy.wait()

    lane = lax.broadcasted_iota(jnp.int32, (LANES - used + 1, local), 0)
    design_t = jnp.concatenate(
        [c_ref[...].astype(F32), jnp.where(lane == 0, 1.0, 0.0)], axis=0
    )
    design[...] = design_t.T.astype(BF16)
    design_t = design_t[: -(-used // 16) * 16].astype(BF16)
    n_t, n_g = share // LANES, width // LANES
    n_blocks = n_t + n_g + 1
    whole, rest = used // 8, used % 8
    strips = -(-used // 8)

    def spot(c, r):
        at = c * rest + r
        return n_blocks * whole + at // 8, at % 8

    for i in range(n_blocks * whole, parts.shape[0]):
        parts[i] = jnp.zeros((8, LANES), F32)
    dose = g_ref[...].astype(F32)
    first = 0
    for block in (
        t_ref[:, pl.ds(pl.multiple_of(my_tile * share, LANES), share)],
        dose.astype(BF16),
        design[...],
    ):
        block = jnp.dot(design_t, block, preferred_element_type=F32)
        for c in range(block.shape[1] // LANES):
            at = slice(LANES * c, LANES * c + LANES)
            for r in range(whole):
                parts[(first + c) * whole + r] = block[8 * r : 8 * r + 8, at]
            for r in range(rest):
                slot, row = spot(first + c, r)
                parts[slot, row : row + 1, :] = block[8 * whole + r : 8 * whole + r + 1, at]
        first += block.shape[1] // LANES

    def source(p, stage):
        return bufs[2 * p * bits + 2 * stage]

    def target(p, stage):
        return bufs[2 * p * bits + 2 * stage + 1]

    def side(p, stage):
        bit = areas[p][0][stage]
        return lax.rem(me // 2**bit, 2), 2**bit

    def copy_of(k, p, stage):
        b, far = side(p, stage)
        return pltpu.make_async_remote_copy(
            src_ref=source(p, stage).at[k, 1 - b],
            dst_ref=target(p, stage).at[k],
            send_sem=send.at[k, p, stage],
            recv_sem=recv.at[k, p, stage],
            device_id={"samp": me + (1 - 2 * b) * far},
            device_id_type=MESH,
        )

    def begin(k):
        for p in range(n_parts):
            copy_of(k, p, 0).start()

    def advance(k, stage):
        for p in range(n_parts):
            copy_of(k, p, stage).wait_recv()
            b, _ = side(p, stage)
            total = source(p, stage)[k, b] + target(p, stage)[k]
            if stage < bits - 1:
                source(p, stage + 1)[k] = total.reshape(source(p, stage + 1).shape[1:])
                copy_of(k, p, stage + 1).start()
            else:
                found[k, areas[p][1], areas[p][2]] = total[0]

    def cross(k, right):
        batch = max(groups // 4, 1)
        for q in range(groups // batch):
            rows = batch * own
            block = jnp.dot(
                rt[q * rows : (q + 1) * rows, :], right, preferred_element_type=F32
            )
            for i in range(batch):
                for p in range(n_parts):
                    order, part_rows, part_lanes = areas[p]
                    lead, other = place_of(order, q * batch + i)
                    source(p, 0)[k, lead, other] = block[i * own : (i + 1) * own][
                        part_rows, part_lanes
                    ]

    def permute(k, rows):
        order = order_ref[pl.ds(k - 1, 1), :] - me * local
        for i in range(local // step):
            row = lax.broadcasted_iota(jnp.int32, (step, local), 0) + i * step
            hot = jnp.where(row == order, 1.0, 0.0).astype(BF16)
            moved[i * step : (i + 1) * step, : rows.shape[1]] = jnp.dot(
                hot, rows, preferred_element_type=F32
            ).astype(BF16)

    step = min(256, local)
    for i in range(local // step):
        at = slice(i * step, (i + 1) * step)
        rt[:, at] = t_ref[at, :].T
    cross(0, (dose - 1.0).astype(BF16))
    pl.semaphore_wait(barrier, groups + tiles - 2)

    def sum_copy(d, source, target, stage):
        return pltpu.make_async_remote_copy(
            src_ref=source,
            dst_ref=target,
            send_sem=sum_sems.at[2 * stage, d - 1],
            recv_sem=sum_sems.at[2 * stage + 1, d - 1],
            device_id=samp_peer(d),
            device_id_type=MESH,
        )

    scattered = [
        sum_copy(d, parts.at[pl.ds(lax.rem(me + d, groups) * quota, quota)], landed.at[d - 1], 0)
        for d in range(1, groups)
    ]
    for copy in scattered:
        copy.start()
    begin(0)
    permute(1, jnp.concatenate([dose.astype(BF16), design[...]], axis=1))
    total = parts[pl.ds(me * quota, quota)]
    for d in range(1, groups):
        scattered[d - 1].wait_recv()
        total = total + landed[d - 1]
    mine[...] = total
    full[my_tile, pl.ds(me * quota, quota)] = total
    gathered = [
        sum_copy(d, mine, full.at[my_tile, pl.ds(me * quota, quota)], 1)
        for d in range(1, groups)
    ]
    for copy in gathered:
        copy.start()
    rhs[...] = jnp.zeros(rhs.shape, F32)
    gram_ref[...] = jnp.zeros(gram_ref.shape, F32)
    coef[...] = jnp.zeros(coef.shape, BF16)
    advance(0, 0)
    for copy in gathered:
        copy.wait_recv()

    def spread_copy(d):
        return pltpu.make_async_remote_copy(
            src_ref=full.at[my_tile],
            dst_ref=full.at[my_tile],
            send_sem=tile_send.at[tiles - 1 + d - 1],
            recv_sem=tile_recv.at[tiles - 1 + d - 1],
            device_id=tile_peer(d),
            device_id_type=MESH,
        )

    spread = [spread_copy(d) for d in range(1, tiles)]
    for copy in spread:
        copy.start()

    half = LANES // 2
    last = n_blocks - 1
    for r in range(whole):
        gram_ref[8 * r : 8 * r + 8, :] = full[my_tile, last * whole + r]
    for r in range(rest):
        slot, row = spot(last, r)
        gram_ref[8 * whole + r : 8 * whole + r + 1, :] = full[my_tile, slot, row : row + 1, :]
    gram = gram_ref[: 8 * strips, :]
    sub = lax.broadcasted_iota(jnp.int32, gram.shape, 0)
    lane = lax.broadcasted_iota(jnp.int32, gram.shape, 1)
    gram = jnp.where(lane == sub + half, 1.0, gram)
    for j in range(used):
        row = gram[j : j + 1, :] * (1.0 / gram[j : j + 1, j : j + 1])
        gram = jnp.where(sub == j, row, gram - gram[:, j : j + 1] * row)
    inverse = jnp.where(lane >= half, gram, 0.0)
    for copy in spread:
        copy.wait_recv()
    for tile in range(tiles + 1):
        held = full.at[tile] if tile < tiles else full.at[my_tile]
        for c in range(n_t if tile < tiles else n_g):
            block = c + (0 if tile < tiles else n_t)
            at = LANES * (tile * n_t + c)
            for r in range(whole):
                rhs[half + 8 * r : half + 8 * r + 8, at : at + LANES] = held[block * whole + r]
            for r in range(rest):
                slot, row = spot(block, r)
                to = half + 8 * whole + r
                rhs[to : to + 1, at : at + LANES] = held[slot, row : row + 1, :]
    coef[: 8 * strips, :] = jnp.dot(
        inverse, rhs[...], precision=HIGHEST, preferred_element_type=F32
    ).astype(BF16)

    advance(0, 1)
    sq_t = jnp.zeros((1, traits), F32)
    for i in range(local // step):
        at = slice(i * step, (i + 1) * step)
        resid = t_ref[at, :].astype(F32) - jnp.dot(
            design[at, :], coef[:, :traits], preferred_element_type=F32
        )
        sq_t = sq_t + jnp.sum(resid * resid, axis=0, keepdims=True)
        rt[:, at] = resid.astype(BF16).T
    resid = moved[:, :width].astype(F32) - jnp.dot(
        moved[:, width:], coef[:, traits:], preferred_element_type=F32
    )
    cross(1, resid.astype(BF16))
    begin(1)
    advance(0, 2)
    sq_g = jnp.zeros((1, width), F32)
    for i in range(local // step):
        at = slice(i * step, (i + 1) * step)
        resid = g_ref[at, :].astype(F32) - jnp.dot(
            design[at, :], coef[:, traits:], preferred_element_type=F32
        )
        sq_g = sq_g + jnp.sum(resid * resid, axis=0, keepdims=True)
        rg[at, :] = resid.astype(BF16)

    def note_squares():
        for j in range(groups):
            at = j * own // LANES * LANES
            notes[j, 0:1, :] = sq_t[:, at : at + LANES]
            for c in range(n_g):
                notes[j, 1 + c : 2 + c, :] = sq_g[:, c * LANES : (c + 1) * LANES]
            if n_g < 7:
                notes[j, 1 + n_g :, :] = jnp.zeros((7 - n_g, LANES), F32)

    def square_copy(d):
        return pltpu.make_async_remote_copy(
            src_ref=notes.at[lax.rem(me + d, groups)],
            dst_ref=squares.at[d],
            send_sem=sq_send.at[d - 1],
            recv_sem=sq_recv.at[d - 1],
            device_id=samp_peer(d),
            device_id_type=MESH,
        )

    note_squares()
    squares[0] = notes[me]
    for d in range(1, groups):
        square_copy(d).start()

    lead = pl.multiple_of(me * own // LANES * LANES, LANES)
    shift = pl.multiple_of(lax.rem(me * own, LANES), 8)

    def correct():
        gram = gram_ref[...]
        lane = lax.broadcasted_iota(jnp.int32, gram.shape, 1)
        gram = jnp.where(lane < half, gram, 0.0)
        coef_g = coef[:, traits:].astype(F32)
        miss = rhs[half:, traits:] - jnp.dot(
            gram, coef_g, precision=HIGHEST, preferred_element_type=F32
        )
        sub = lax.broadcasted_iota(jnp.int32, (half, width), 0)
        fit = coef_g[:half] - jnp.where(sub == used - 1, 1.0, 0.0)
        left = jnp.concatenate(
            [rhs[half:, pl.ds(lead, LANES)], coef[:half, pl.ds(lead, LANES)].astype(F32)], axis=0
        )
        column[...] = left.T
        fix[...] = jnp.dot(
            column[pl.ds(shift, own), :],
            jnp.concatenate([fit, miss], axis=0),
            precision=HIGHEST,
            preferred_element_type=F32,
        )

    correct()

    def turn(t, carry):
        @pl.when(t < turns)
        def _():
            permute(t, rg[...])
            cross(t, moved[:, :width])
            begin(t)

        for stage in range(bits):
            k = t - 1 - stage

            @pl.when(jnp.logical_and(k >= (0 if stage > 2 else 1), k < turns))
            def _():
                advance(k, stage)

        return carry

    lax.fori_loop(2, turns + bits, turn, 0)

    total = squares[0]
    for d in range(1, groups):
        square_copy(d).wait_recv()
        total = total + squares[d]
    gain = lax.rsqrt(total / samples + epsilon)
    factor = math.sqrt(samples - used - 1) / samples
    gain_g = jnp.concatenate([gain[1 + c : 2 + c, :] for c in range(n_g)], axis=1)
    column[...] = jnp.broadcast_to(gain.T[:, :1] * factor, column.shape)
    gain_t = column[pl.ds(shift, own), :]
    gain_t = gain_t[:, :1]
    score_ref[...] = (found[0] - fix[...]) * gain_g * gain_t
    top = jnp.zeros((own, LANES), F32)
    pos = lax.broadcasted_iota(jnp.int32, top.shape, 1)
    for k in range(1, turns):
        peak = jnp.max(jnp.abs(found[k] * gain_g), axis=1, keepdims=True) * gain_t
        top = jnp.where(pos == k - 1, peak, top)
    peaks[0] = top
    crossed = [
        pltpu.make_async_remote_copy(
            src_ref=peaks.at[0],
            dst_ref=peaks.at[d],
            send_sem=tile_send.at[d - 1],
            recv_sem=tile_recv.at[d - 1],
            device_id=tile_peer(d),
            device_id_type=MESH,
        )
        for d in range(1, tiles)
    ]
    for copy in crossed:
        copy.start()
    for copy in scattered + gathered + spread:
        copy.wait_send()

    def finish(k, carry):
        for p in range(n_parts):
            for stage in range(bits):
                copy_of(k, p, stage).wait_send()
        return carry

    lax.fori_loop(0, turns, finish, 0)
    for d in range(1, groups):
        square_copy(d).wait_send()
    for d in range(1, tiles):
        crossed[d - 1].wait()
        top = jnp.maximum(top, peaks[d])
    peak_ref[...] = top.T[: turns - 1]


def shards(traits, covariates, genotypes, shuffles):
    groups, tiles = lax.axis_size("samp"), lax.axis_size("tile")
    bits = groups.bit_length() - 1
    turns = shuffles.shape[0] + 1
    local, n_traits = traits.shape
    width = genotypes.shape[1]
    used = covariates.shape[1] + 1
    own = n_traits // groups
    areas = parts_of(bits, own, width)
    bufs = []
    for _, part_rows, part_lanes in areas:
        size = (part_rows.stop - part_rows.start, part_lanes.stop - part_lanes.start)
        for stage in range(bits):
            lot = 2 ** (bits - 1 - stage)
            bufs.append(pltpu.VMEM((turns, 2, lot) + size, F32))
            bufs.append(pltpu.VMEM((turns, lot) + size, F32))
    n_blocks = (n_traits // tiles + width) // LANES + 1
    slots = n_blocks * (used // 8) + -(-n_blocks * (used % 8) // 8)
    quota = -(-slots // groups)
    vmem = pl.BlockSpec(memory_space=pltpu.VMEM)
    sems = pltpu.SemaphoreType.DMA((turns, len(areas), bits))
    flat = pltpu.SemaphoreType.DMA((groups - 1,))
    pair = pltpu.SemaphoreType.DMA((max(2 * (tiles - 1), 1),))
    return pl.pallas_call(
        functools.partial(scan_kernel, groups, tiles, local * groups, used, areas),
        out_shape=(
            pltpu.VMEM((own, width), F32),
            pltpu.VMEM((turns - 1, own), F32),
        ),
        in_specs=[pl.BlockSpec(memory_space=pl.ANY)] * 4,
        out_specs=(vmem, vmem),
        scratch_shapes=[
            pltpu.VMEM((local, n_traits), BF16),
            pltpu.VMEM((used - 1, local), BF16),
            pltpu.VMEM((local, width), jnp.int32),
            pltpu.VMEM((turns - 1, local), jnp.int32),
            pltpu.SemaphoreType.DMA((4,)),
            pltpu.VMEM((local, LANES), BF16),
            pltpu.VMEM((quota * groups, 8, LANES), F32),
            pltpu.VMEM((groups - 1, quota, 8, LANES), F32),
            pltpu.VMEM((quota, 8, LANES), F32),
            pltpu.VMEM((tiles, quota * groups, 8, LANES), F32),
            pltpu.VMEM((LANES, n_traits + width), F32),
            pltpu.VMEM((LANES, n_traits + width), BF16),
            pltpu.VMEM((n_traits, local), BF16),
            pltpu.VMEM((local, width), BF16),
            pltpu.VMEM((local, width + LANES), BF16),
            pltpu.VMEM((turns, own, width), F32),
            pltpu.VMEM((own, width), F32),
            pltpu.VMEM((LANES // 2, LANES), F32),
            pltpu.VMEM((groups, 8, LANES), F32),
            pltpu.VMEM((groups, 8, LANES), F32),
            pltpu.VMEM((LANES, LANES), F32),
            pltpu.VMEM((tiles, own, LANES), F32),
            pltpu.SemaphoreType.DMA((4, groups - 1)),
            flat,
            flat,
            pair,
            pair,
            sems,
            sems,
            *bufs,
        ],
        compiler_params=pltpu.CompilerParams(
            collective_id=0, has_side_effects=True, vmem_limit_bytes=60 * 1024 * 1024
        ),
        name="scan",
    )(traits, covariates.T, genotypes, shuffles)


def solution(mesh):
    placed = (P("samp", None), P("samp", None), P("samp", "tile"), P(None, "samp"))
    return jax.shard_map(
        shards,
        mesh=mesh,
        in_specs=placed,
        out_specs=(P("samp", "tile"), P(None, "samp")),
        check_vma=False,
    )
```

```python
import functools
import math

import jax
import jax.numpy as jnp
from jax import lax
from jax.experimental import pallas as pl
from jax.experimental.pallas import tpu as pltpu
from jax.sharding import PartitionSpec as P

MESH = pl.DeviceIdType.MESH
LANES = 128
F32, BF16 = jnp.float32, jnp.bfloat16
HIGHEST = lax.Precision.HIGHEST
epsilon = 1e-05


def parts_of(bits, own, width):
    cut, half = own - max(8, own // 32 * 8), width // 2
    mid = (cut // 8 + 1) // 2 * 8
    ones = tuple((bit,) for bit in range(bits))
    far = ones[2:-2] + ((bits - 2, bits - 1),)
    x_first, y_first = ones[:2] + far, ones[1::-1] + far
    return (
        (x_first, slice(0, mid), slice(0, half)),
        (y_first, slice(0, mid), slice(half, width)),
        (ones[2:] + ones[:2], slice(cut, own), slice(0, half)),
        (ones[2::-1] + ones[3:], slice(cut, own), slice(half, width)),
        (x_first, slice(mid, cut), slice(0, half)),
        (y_first, slice(mid, cut), slice(half, width)),
    )


HALVES = ((0, 1, 2, 3), (4, 5))


def place_of(order, g):
    at = [g >> some[0] & 2 ** len(some) - 1 for some in order]
    rest = 0
    for digit, some in zip(at[1:], order[1:]):
        rest = 2 ** len(some) * rest + digit
    return at[0], rest


def scan_kernel(
    groups, tiles, samples, used, areas, t_hbm, c_hbm, g_hbm, order_hbm, score_ref, peak_ref,
    t_ref, c_ref, g_ref, order_ref, load, design, parts, landed, mine, full, rhs, coef, rt, rg,
    moved, found, fix, gram_part, gram_landed, gram_sum, gram_ref, notes, squares, column, gain_g,
    peaks, flat, tile_send, tile_recv, send, recv, *bufs
):
    me = lax.axis_index("samp")
    my_tile = lax.axis_index("tile")
    turns, width, n_parts = found.shape[0], found.shape[2], len(areas)
    bits = groups.bit_length() - 1
    local, traits = t_ref.shape
    own = traits // groups
    share = traits // tiles
    quota = parts.shape[0] // groups

    def samp_peer(d):
        return {"samp": lax.rem(me + d, groups)}

    def tile_peer(d):
        return {"tile": lax.rem(my_tile + d, tiles)}

    barrier = pltpu.get_barrier_semaphore()
    for d in range(1, groups):
        pl.semaphore_signal(barrier, inc=1, device_id=samp_peer(d), device_id_type=MESH)
    for d in range(1, tiles):
        pl.semaphore_signal(barrier, inc=1, device_id=tile_peer(d), device_id_type=MESH)
    loads = [
        pltpu.make_async_copy(a, b, load.at[i])
        for i, (a, b) in enumerate(
            ((c_hbm, c_ref), (t_hbm, t_ref), (g_hbm, g_ref), (order_hbm, order_ref))
        )
    ]
    for copy in loads:
        copy.start()
    for copy in loads:
        copy.wait()

    lane = lax.broadcasted_iota(jnp.int32, (LANES - used + 1, local), 0)
    design_t = jnp.concatenate(
        [c_ref[...].astype(F32), jnp.where(lane == 0, 1.0, 0.0)], axis=0
    )
    design[...] = design_t.T.astype(BF16)
    design_t = design_t[: -(-used // 16) * 16].astype(BF16)
    n_t, n_g = share // LANES, width // LANES
    n_blocks = n_t + n_g
    whole, rest = used // 8, used % 8
    strips = -(-used // 8)

    def spot(c, r):
        at = c * rest + r
        return n_blocks * whole + at // 8, at % 8

    for i in range(n_blocks * whole, parts.shape[0]):
        parts[i] = jnp.zeros((8, LANES), F32)
    dose = g_ref[...].astype(F32)
    first = 0
    for block in (
        t_ref[:, pl.ds(pl.multiple_of(my_tile * share, LANES), share)],
        dose.astype(BF16),
    ):
        block = jnp.dot(design_t, block, preferred_element_type=F32)
        for c in range(block.shape[1] // LANES):
            at = slice(LANES * c, LANES * c + LANES)
            for r in range(whole):
                parts[(first + c) * whole + r] = block[8 * r : 8 * r + 8, at]
            for r in range(rest):
                slot, row = spot(first + c, r)
                parts[slot, row : row + 1, :] = block[8 * whole + r : 8 * whole + r + 1, at]
        first += block.shape[1] // LANES

    gram = jnp.dot(design_t, design[...], preferred_element_type=F32)
    gram_part[...] = jnp.zeros(gram_part.shape, F32)
    lots = gram_part.shape[1]
    pack = LANES // (8 * strips)
    for r in range(strips):
        at = slice(r % pack * 8 * strips, (r % pack + 1) * 8 * strips)
        gram_part[r // pack // lots, r // pack % lots, :, at] = gram[
            8 * r : 8 * r + 8, : 8 * strips
        ]

    def await_all(sem, like):
        pltpu.make_async_copy(like, like, flat.at[sem]).wait()

    starts = [sum(2 * len(area[0]) for area in areas[:p]) for p in range(n_parts)]

    def source(p, stage):
        return bufs[starts[p] + 2 * stage]

    def target(p, stage):
        return bufs[starts[p] + 2 * stage + 1]

    def digit(p, stage):
        some = areas[p][0][stage]
        return lax.rem(me // 2 ** some[0], 2 ** len(some)), 2 ** len(some), 2 ** some[0]

    def copies(k, p, stage):
        mine, n, far = digit(p, stage)
        first = sum(2 ** len(some) - 1 for some in areas[p][0][:stage])
        out = []
        for d in range(1, n):
            other = lax.rem(mine + d, n)
            at = lax.rem(k, 2), p, first + d - 1
            out.append(
                pltpu.make_async_remote_copy(
                    src_ref=source(p, stage).at[k, other],
                    dst_ref=target(p, stage).at[k, d - 1],
                    send_sem=send.at[at],
                    recv_sem=recv.at[at],
                    device_id={"samp": me + (other - mine) * far},
                    device_id_type=MESH,
                )
            )
        return out

    def begin(k, part):
        for p in HALVES[part]:
            for copy in copies(k, p, 0):
                copy.start()

    def advance(k, part, stage, first=False):
        for p in HALVES[part]:
            if stage >= len(areas[p][0]):
                continue
            for copy in copies(k, p, stage):
                copy.wait_recv()
            if not first:
                for copy in copies(k - 1, p, stage):
                    copy.wait_send()
            mine, n, _ = digit(p, stage)
            total = source(p, stage)[k, mine]
            for d in range(1, n):
                total = total + target(p, stage)[k, d - 1]
            if stage < len(areas[p][0]) - 1:
                source(p, stage + 1)[k] = total.reshape(source(p, stage + 1).shape[1:])
                for copy in copies(k, p, stage + 1):
                    copy.start()
            else:
                found[k, areas[p][1], areas[p][2]] = total[0]

    def cross(k, right):
        batch = max(groups // 4, 1)
        for q in range(groups // batch):
            rows = batch * own
            block = jnp.dot(
                rt[q * rows : (q + 1) * rows, :], right, preferred_element_type=F32
            )
            for i in range(batch):
                for p in range(n_parts):
                    order, part_rows, part_lanes = areas[p]
                    lead, other = place_of(order, q * batch + i)
                    source(p, 0)[k, lead, other] = block[i * own : (i + 1) * own][
                        part_rows, part_lanes
                    ]

    pl.semaphore_wait(barrier, groups + tiles - 2)

    odd = lax.rem(my_tile, 2)

    def gram_copy(d):
        return pltpu.make_async_remote_copy(
            src_ref=gram_part.at[odd],
            dst_ref=gram_landed.at[d - 1],
            send_sem=flat.at[4],
            recv_sem=flat.at[5],
            device_id=samp_peer(d),
            device_id_type=MESH,
        )

    for d in range(1, groups):
        gram_copy(d).start()

    def sum_copy(d, source, target, stage):
        return pltpu.make_async_remote_copy(
            src_ref=source,
            dst_ref=target,
            send_sem=flat.at[2 * stage],
            recv_sem=flat.at[2 * stage + 1],
            device_id=samp_peer(d),
            device_id_type=MESH,
        )

    scattered = [
        sum_copy(d, parts.at[pl.ds(lax.rem(me + d, groups) * quota, quota)], landed.at[d - 1], 0)
        for d in range(1, groups)
    ]
    for copy in scattered:
        copy.start()
    def permute(k, rows):
        order = order_ref[pl.ds(k - 1, 1), :] - me * local
        for i in range(local // step):
            row = lax.broadcasted_iota(jnp.int32, (step, local), 0) + i * step
            hot = jnp.where(row == order, 1.0, 0.0).astype(BF16)
            moved[i * step : (i + 1) * step, : rows.shape[1]] = jnp.dot(
                hot, rows, preferred_element_type=F32
            ).astype(BF16)

    step = min(256, local)
    for i in range(local // step):
        at = slice(i * step, (i + 1) * step)
        rt[:, at] = t_ref[at, :].T
    cross(0, (dose - 1.0).astype(BF16))
    begin(0, 0)
    begin(0, 1)
    permute(1, jnp.concatenate([dose.astype(BF16), design[...]], axis=1))
    total = parts[pl.ds(me * quota, quota)]
    await_all(1, landed)
    for d in range(1, groups):
        total = total + landed[d - 1]
    mine[...] = total
    full[my_tile, pl.ds(me * quota, quota)] = total
    gathered = [
        sum_copy(d, mine, full.at[my_tile, pl.ds(me * quota, quota)], 1)
        for d in range(1, groups)
    ]
    for copy in gathered:
        copy.start()
    await_all(5, gram_landed)
    total = gram_part[odd]
    for d in range(1, groups):
        total = total + gram_landed[d - 1]
    gram_sum[odd] = total
    swap = pltpu.make_async_remote_copy(
        src_ref=gram_sum.at[odd],
        dst_ref=gram_sum.at[odd],
        send_sem=tile_send.at[2 * (tiles - 1)],
        recv_sem=tile_recv.at[2 * (tiles - 1)],
        device_id={"tile": my_tile + 1 - 2 * odd},
        device_id_type=MESH,
    )
    swap.start()
    rhs[...] = jnp.zeros(rhs.shape, F32)
    gram_ref[...] = jnp.zeros(gram_ref.shape, F32)
    coef[...] = jnp.zeros(coef.shape, BF16)
    half = LANES // 2
    swap.wait_recv()
    for r in range(strips):
        at = slice(r % pack * 8 * strips, (r % pack + 1) * 8 * strips)
        gram_ref[8 * r : 8 * r + 8, : 8 * strips] = gram_sum[r // pack // lots, r // pack % lots][
            :, at
        ]
    gram = gram_ref[: 8 * strips, :]
    sub = lax.broadcasted_iota(jnp.int32, gram.shape, 0)
    lane = lax.broadcasted_iota(jnp.int32, gram.shape, 1)
    gram = jnp.where(lane == sub + half, 1.0, gram)
    for j in range(used):
        row = gram[j : j + 1, :] * (1.0 / gram[j : j + 1, j : j + 1])
        gram = jnp.where(sub == j, row, gram - gram[:, j : j + 1] * row)
    inverse = jnp.where(lane >= half, gram, 0.0)
    advance(0, 0, 0, True)
    advance(0, 1, 0, True)
    await_all(3, landed)

    def spread_copy(d):
        return pltpu.make_async_remote_copy(
            src_ref=full.at[my_tile],
            dst_ref=full.at[my_tile],
            send_sem=tile_send.at[tiles - 1 + d - 1],
            recv_sem=tile_recv.at[tiles - 1 + d - 1],
            device_id=tile_peer(d),
            device_id_type=MESH,
        )

    spread = [spread_copy(d) for d in range(1, tiles)]
    for copy in spread:
        copy.start()

    for copy in spread:
        copy.wait_recv()
    for tile in range(tiles + 1):
        held = full.at[tile] if tile < tiles else full.at[my_tile]
        for c in range(n_t if tile < tiles else n_g):
            block = c + (0 if tile < tiles else n_t)
            at = LANES * (tile * n_t + c)
            for r in range(whole):
                rhs[half + 8 * r : half + 8 * r + 8, at : at + LANES] = held[block * whole + r]
            for r in range(rest):
                slot, row = spot(block, r)
                to = half + 8 * whole + r
                rhs[to : to + 1, at : at + LANES] = held[slot, row : row + 1, :]
    coef[: 8 * strips, :] = jnp.dot(
        inverse, rhs[...], precision=HIGHEST, preferred_element_type=F32
    ).astype(BF16)

    advance(0, 0, 1, True)
    advance(0, 1, 1, True)
    sq_t = jnp.zeros((1, traits), F32)
    for i in range(local // step):
        at = slice(i * step, (i + 1) * step)
        resid = t_ref[at, :].astype(F32) - jnp.dot(
            design[at, :], coef[:, :traits], preferred_element_type=F32
        )
        sq_t = sq_t + jnp.sum(resid * resid, axis=0, keepdims=True)
        rt[:, at] = resid.astype(BF16).T
    resid = moved[:, :width].astype(F32) - jnp.dot(
        moved[:, width:], coef[:, traits:], preferred_element_type=F32
    )
    cross(1, resid.astype(BF16))
    begin(1, 0)
    begin(1, 1)
    advance(0, 0, 2, True)
    advance(0, 1, 2, True)
    sq_g = jnp.zeros((1, width), F32)
    for i in range(local // step):
        at = slice(i * step, (i + 1) * step)
        resid = g_ref[at, :].astype(F32) - jnp.dot(
            design[at, :], coef[:, traits:], preferred_element_type=F32
        )
        sq_g = sq_g + jnp.sum(resid * resid, axis=0, keepdims=True)
        rg[at, :] = resid.astype(BF16)

    def note_squares():
        for j in range(groups):
            at = j * own // LANES * LANES
            notes[j, 0:1, :] = sq_t[:, at : at + LANES]
            for c in range(n_g):
                notes[j, 1 + c : 2 + c, :] = sq_g[:, c * LANES : (c + 1) * LANES]
            if n_g < 7:
                notes[j, 1 + n_g :, :] = jnp.zeros((7 - n_g, LANES), F32)

    def square_copy(d):
        return pltpu.make_async_remote_copy(
            src_ref=notes.at[lax.rem(me + d, groups)],
            dst_ref=squares.at[d],
            send_sem=flat.at[6],
            recv_sem=flat.at[7],
            device_id=samp_peer(d),
            device_id_type=MESH,
        )

    note_squares()
    squares[0] = notes[me]
    for d in range(1, groups):
        square_copy(d).start()

    lead = pl.multiple_of(me * own // LANES * LANES, LANES)
    shift = pl.multiple_of(lax.rem(me * own, LANES), 8)

    def correct():
        gram = gram_ref[...]
        lane = lax.broadcasted_iota(jnp.int32, gram.shape, 1)
        gram = jnp.where(lane < half, gram, 0.0)
        coef_g = coef[:, traits:].astype(F32)
        miss = rhs[half:, traits:] - jnp.dot(
            gram, coef_g, precision=HIGHEST, preferred_element_type=F32
        )
        sub = lax.broadcasted_iota(jnp.int32, (half, width), 0)
        fit = coef_g[:half] - jnp.where(sub == used - 1, 1.0, 0.0)
        left = jnp.concatenate(
            [rhs[half:, pl.ds(lead, LANES)], coef[:half, pl.ds(lead, LANES)].astype(F32)], axis=0
        )
        column[...] = left.T
        fix[...] = jnp.dot(
            column[pl.ds(shift, own), :],
            jnp.concatenate([fit, miss], axis=0),
            precision=HIGHEST,
            preferred_element_type=F32,
        )

    correct()

    peaks[0] = jnp.zeros(peaks.shape[1:], F32)

    def scale():
        total = squares[0]
        await_all(7, squares.at[pl.ds(1, groups - 1)])
        for d in range(1, groups):
            total = total + squares[d]
        gain = lax.rsqrt(total / samples + epsilon)
        factor = math.sqrt(samples - used - 1) / samples
        for c in range(n_g):
            gain_g[:, c * LANES : (c + 1) * LANES] = jnp.broadcast_to(
                gain[1 + c : 2 + c, :], (8, LANES)
            )
        column[...] = jnp.broadcast_to(gain.T[:, :1] * factor, column.shape)

    def peak_of(k):
        gain_t = column[pl.ds(shift, own), :]
        peak = jnp.max(jnp.abs(found[k] * gain_g[:1, :]), axis=1, keepdims=True) * gain_t
        pos = lax.broadcasted_iota(jnp.int32, peak.shape, 1)
        peaks[0] = jnp.where(pos == k - 1, peak, peaks[0])

    def turn(t, carry):
        for stage in range(3, bits):

            @pl.when(t == stage - 1)
            def _():
                advance(0, 0, stage, True)
                advance(0, 1, stage, True)

        fresh = jnp.logical_and(t > 1, t < turns)

        @pl.when(fresh)
        def _():
            begin(t, 0)

        @pl.when(t + 1 < turns)
        def _():
            permute(t + 1, rg[...])
            cross(t + 1, moved[:, :width])

        for part in range(2):
            if part == 1:

                @pl.when(fresh)
                def _():
                    begin(t, 1)

            for stage in range(bits):
                back = part - 1 - stage
                k = t + back // 2

                @pl.when(jnp.logical_and(k > 0, k < turns))
                def _():
                    advance(k, back % 2, stage)

        @pl.when(t == 2)
        def _():
            scale()

        k = t - (bits + 1) // 2

        @pl.when(k == 0)
        def _():
            score_ref[...] = (
                (found[0] - fix[...]) * gain_g[:1, :] * column[pl.ds(shift, own), :][:, :1]
            )

        @pl.when(k > 0)
        def _():
            peak_of(k)

        return carry

    lax.fori_loop(1, turns + (bits + 1) // 2, turn, 0)
    crossed = [
        pltpu.make_async_remote_copy(
            src_ref=peaks.at[0],
            dst_ref=peaks.at[d],
            send_sem=tile_send.at[d - 1],
            recv_sem=tile_recv.at[d - 1],
            device_id=tile_peer(d),
            device_id_type=MESH,
        )
        for d in range(1, tiles)
    ]
    for copy in crossed:
        copy.start()
    for copy in spread + [swap]:
        copy.wait_send()
    await_all(0, landed)
    await_all(2, landed)
    await_all(4, gram_landed)
    await_all(6, squares.at[pl.ds(1, groups - 1)])
    for p in range(n_parts):
        for stage in range(len(areas[p][0])):
            for copy in copies(turns - 1, p, stage):
                copy.wait_send()
    top = peaks[0]
    for d in range(1, tiles):
        crossed[d - 1].wait()
        top = jnp.maximum(top, peaks[d])
    peak_ref[...] = top.T[: turns - 1]


def shards(traits, covariates, genotypes, shuffles):
    groups, tiles = lax.axis_size("samp"), lax.axis_size("tile")
    bits = groups.bit_length() - 1
    turns = shuffles.shape[0] + 1
    local, n_traits = traits.shape
    width = genotypes.shape[1]
    used = covariates.shape[1] + 1
    own = n_traits // groups
    areas = parts_of(bits, own, width)
    bufs = []
    for order, part_rows, part_lanes in areas:
        size = (part_rows.stop - part_rows.start, part_lanes.stop - part_lanes.start)
        lot = groups
        for some in order:
            n = 2 ** len(some)
            lot //= n
            bufs.append(pltpu.VMEM((turns, n, lot) + size, F32))
            bufs.append(pltpu.VMEM((turns, n - 1, lot) + size, F32))
    n_blocks = (n_traits // tiles + width) // LANES
    strips = -(-used // 8)
    lots = -(-strips // (LANES // (8 * strips) * 2))
    slots = n_blocks * (used // 8) + -(-n_blocks * (used % 8) // 8)
    quota = -(-slots // groups)
    vmem = pl.BlockSpec(memory_space=pltpu.VMEM)
    sems = pltpu.SemaphoreType.DMA((2, len(areas), bits + 1))
    pair = pltpu.SemaphoreType.DMA((2 * tiles - 1,))
    return pl.pallas_call(
        functools.partial(scan_kernel, groups, tiles, local * groups, used, areas),
        out_shape=(
            pltpu.VMEM((own, width), F32),
            pltpu.VMEM((turns - 1, own), F32),
        ),
        in_specs=[pl.BlockSpec(memory_space=pl.ANY)] * 4,
        out_specs=(vmem, vmem),
        scratch_shapes=[
            pltpu.VMEM((local, n_traits), BF16),
            pltpu.VMEM((used - 1, local), BF16),
            pltpu.VMEM((local, width), jnp.int32),
            pltpu.VMEM((turns - 1, local), jnp.int32),
            pltpu.SemaphoreType.DMA((4,)),
            pltpu.VMEM((local, LANES), BF16),
            pltpu.VMEM((quota * groups, 8, LANES), F32),
            pltpu.VMEM((groups - 1, quota, 8, LANES), F32),
            pltpu.VMEM((quota, 8, LANES), F32),
            pltpu.VMEM((tiles, quota * groups, 8, LANES), F32),
            pltpu.VMEM((LANES, n_traits + width), F32),
            pltpu.VMEM((LANES, n_traits + width), BF16),
            pltpu.VMEM((n_traits, local), BF16),
            pltpu.VMEM((local, width), BF16),
            pltpu.VMEM((local, width + LANES), BF16),
            pltpu.VMEM((turns, own, width), F32),
            pltpu.VMEM((own, width), F32),
            pltpu.VMEM((2, lots, 8, LANES), F32),
            pltpu.VMEM((groups - 1, lots, 8, LANES), F32),
            pltpu.VMEM((2, lots, 8, LANES), F32),
            pltpu.VMEM((LANES // 2, LANES), F32),
            pltpu.VMEM((groups, 8, LANES), F32),
            pltpu.VMEM((groups, 8, LANES), F32),
            pltpu.VMEM((LANES, LANES), F32),
            pltpu.VMEM((8, width), F32),
            pltpu.VMEM((tiles, own, LANES), F32),
            pltpu.SemaphoreType.DMA((8,)),
            pair,
            pair,
            sems,
            sems,
            *bufs,
        ],
        compiler_params=pltpu.CompilerParams(
            collective_id=0, has_side_effects=True, vmem_limit_bytes=60 * 1024 * 1024
        ),
        name="scan",
    )(traits, covariates.T, genotypes, shuffles)


def solution(mesh):
    placed = (P("samp", None), P("samp", None), P("samp", "tile"), P(None, "samp"))
    return jax.shard_map(
        shards,
        mesh=mesh,
        in_specs=placed,
        out_specs=(P("samp", "tile"), P(None, "samp")),
        check_vma=False,
    )
```

```python
import functools
import math

import jax
import jax.numpy as jnp
from jax import lax
from jax.experimental import pallas as pl
from jax.experimental.pallas import tpu as pltpu
from jax.sharding import PartitionSpec as P

MESH = pl.DeviceIdType.MESH
LANES = 128
F32, BF16 = jnp.float32, jnp.bfloat16
HIGHEST = lax.Precision.HIGHEST
epsilon = 1e-05


def parts_of(bits, own, width):
    cut, half = own - max(8, own // 32 * 8), width // 2
    mid = (cut // 8 + 1) // 2 * 8
    ones = tuple((bit,) for bit in range(bits))
    far = ones[2:-2] + ((bits - 2, bits - 1),)
    x_first, y_first = ones[:2] + far, ones[1::-1] + far
    return (
        (x_first, slice(0, mid), slice(0, half)),
        (y_first, slice(0, mid), slice(half, width)),
        (ones[2:] + ones[:2], slice(cut, own), slice(0, half)),
        (ones[2::-1] + ones[3:], slice(cut, own), slice(half, width)),
        (x_first, slice(mid, cut), slice(0, half)),
        (y_first, slice(mid, cut), slice(half, width)),
    )


HALVES = ((0, 1, 2, 3), (4, 5))


def place_of(order, g):
    at = [g >> some[0] & 2 ** len(some) - 1 for some in order]
    rest = 0
    for digit, some in zip(at[1:], order[1:]):
        rest = 2 ** len(some) * rest + digit
    return at[0], rest


def scan_kernel(
    groups, tiles, samples, used, areas, t_hbm, c_hbm, g_hbm, order_hbm, score_ref, peak_ref,
    t_ref, c_ref, g_ref, order_ref, load, design, parts_t, parts_g, landed_t, landed_g, mine, full, rhs, coef, rt, rg,
    moved, found, fix, gram_part, gram_landed, gram_sum, gram_ref, notes, squares, column, gain_g,
    peaks, flat, tile_send, tile_recv, send, recv, *bufs
):
    me = lax.axis_index("samp")
    my_tile = lax.axis_index("tile")
    turns, width, n_parts = found.shape[0], found.shape[2], len(areas)
    bits = groups.bit_length() - 1
    local, traits = t_ref.shape
    own = traits // groups
    pairs = tiles // 2
    share = traits // pairs
    quota_t, quota_g = parts_t.shape[0] // groups, parts_g.shape[0] // groups
    odd, pair = lax.rem(my_tile, 2), my_tile // 2
    other = my_tile + 1 - 2 * odd

    def samp_peer(d):
        return {"samp": lax.rem(me + d, groups)}

    def tile_peer(d):
        return {"tile": lax.rem(my_tile + d, tiles)}

    barrier = pltpu.get_barrier_semaphore()
    for d in range(1, groups):
        pl.semaphore_signal(barrier, inc=1, device_id=samp_peer(d), device_id_type=MESH)
    for d in range(1, tiles):
        pl.semaphore_signal(barrier, inc=1, device_id=tile_peer(d), device_id_type=MESH)
    for d in range(1, groups):
        pl.semaphore_signal(
            barrier,
            inc=1,
            device_id={"samp": lax.rem(me + d, groups), "tile": other},
            device_id_type=MESH,
        )
    chunk = local // 4
    pieces = [(c_hbm, c_ref)]
    for i in range(4):
        at = pl.ds(i * chunk, chunk)
        pieces.append((g_hbm.at[at], g_ref.at[at]))
        pieces.append((t_hbm.at[at], t_ref.at[at]))
    pieces.append((order_hbm, order_ref))
    loads = [pltpu.make_async_copy(a, b, load.at[i]) for i, (a, b) in enumerate(pieces)]
    for copy in loads:
        copy.start()
    for copy in loads:
        copy.wait()

    lane = lax.broadcasted_iota(jnp.int32, (LANES - used + 1, local), 0)
    design_t = jnp.concatenate(
        [c_ref[...].astype(F32), jnp.where(lane == 0, 1.0, 0.0)], axis=0
    )
    design[...] = design_t.T.astype(BF16)
    design_t = design_t[: -(-used // 16) * 16].astype(BF16)
    n_t, n_g = share // LANES, width // LANES
    whole, rest = used // 8, used % 8
    strips = -(-used // 8)

    def spot(c, r):
        at = c * rest + r
        return n_g * whole + at // 8, at % 8

    for i in range(n_g * whole, parts_g.shape[0]):
        parts_g[i] = jnp.zeros((8, LANES), F32)
    dose = g_ref[...].astype(F32)

    def put(block, parts, first):
        for c in range(block.shape[1] // LANES):
            at = slice(LANES * c, LANES * c + LANES)
            for r in range(whole):
                parts[c * whole + r] = block[8 * r : 8 * r + 8, at]
            for r in range(rest):
                slot, row = spot(first + c, r)
                parts_g[slot, row : row + 1, :] = block[8 * whole + r : 8 * whole + r + 1, at]

    put(jnp.dot(design_t, dose.astype(BF16), preferred_element_type=F32), parts_g, n_t)

    @pl.when(odd == 1)
    def _():
        block = t_ref[:, pl.ds(pl.multiple_of(pair * share, LANES), share)]
        put(jnp.dot(design_t, block, preferred_element_type=F32), parts_t, 0)
        for i in range(n_t * whole, parts_t.shape[0]):
            parts_t[i] = jnp.zeros((8, LANES), F32)

    gram = jnp.dot(design_t, design[...], preferred_element_type=F32)
    gram_part[...] = jnp.zeros(gram_part.shape, F32)
    pack = LANES // (8 * strips)
    for r in range(strips):
        at = slice(r % pack * 8 * strips, (r % pack + 1) * 8 * strips)
        gram_part[r // pack, :, at] = gram[8 * r : 8 * r + 8, : 8 * strips]

    def await_all(sem, like):
        pltpu.make_async_copy(like, like, flat.at[sem]).wait()

    starts = [sum(2 * len(area[0]) for area in areas[:p]) for p in range(n_parts)]

    def source(p, stage):
        return bufs[starts[p] + 2 * stage]

    def target(p, stage):
        return bufs[starts[p] + 2 * stage + 1]

    def digit(p, stage):
        some = areas[p][0][stage]
        return lax.rem(me // 2 ** some[0], 2 ** len(some)), 2 ** len(some), 2 ** some[0]

    def copies(k, p, stage):
        mine, n, far = digit(p, stage)
        first = sum(2 ** len(some) - 1 for some in areas[p][0][:stage])
        out = []
        for d in range(1, n):
            other = lax.rem(mine + d, n)
            at = lax.rem(k, 2), p, first + d - 1
            out.append(
                pltpu.make_async_remote_copy(
                    src_ref=source(p, stage).at[k, other],
                    dst_ref=target(p, stage).at[k, d - 1],
                    send_sem=send.at[at],
                    recv_sem=recv.at[at],
                    device_id={"samp": me + (other - mine) * far},
                    device_id_type=MESH,
                )
            )
        return out

    def begin(k, part):
        for p in HALVES[part]:
            for copy in copies(k, p, 0):
                copy.start()

    def advance(k, part, stage, first=False):
        for p in HALVES[part]:
            if stage >= len(areas[p][0]):
                continue
            for copy in copies(k, p, stage):
                copy.wait_recv()
            if not first:
                for copy in copies(k - 1, p, stage):
                    copy.wait_send()
            mine, n, _ = digit(p, stage)
            total = source(p, stage)[k, mine]
            for d in range(1, n):
                total = total + target(p, stage)[k, d - 1]
            if stage < len(areas[p][0]) - 1:
                source(p, stage + 1)[k] = total.reshape(source(p, stage + 1).shape[1:])
                for copy in copies(k, p, stage + 1):
                    copy.start()
            else:
                found[k, areas[p][1], areas[p][2]] = total[0]

    def cross(k, right):
        batch = max(groups // 4, 1)
        for q in range(groups // batch):
            rows = batch * own
            block = jnp.dot(
                rt[q * rows : (q + 1) * rows, :], right, preferred_element_type=F32
            )
            for i in range(batch):
                for p in range(n_parts):
                    order, part_rows, part_lanes = areas[p]
                    lead, other = place_of(order, q * batch + i)
                    source(p, 0)[k, lead, other] = block[i * own : (i + 1) * own][
                        part_rows, part_lanes
                    ]

    pl.semaphore_wait(barrier, 2 * (groups - 1) + tiles - 1)

    def flat_copy(d, source, target, sem, device):
        return pltpu.make_async_remote_copy(
            src_ref=source,
            dst_ref=target,
            send_sem=flat.at[sem],
            recv_sem=flat.at[sem + 1],
            device_id=device,
            device_id_type=MESH,
        )

    def g_copy(d, side, device):
        at = pl.ds(lax.rem(me + d, groups) * quota_g, quota_g)
        return pltpu.make_async_remote_copy(
            src_ref=parts_g.at[at],
            dst_ref=landed_g.at[side, d - 1],
            send_sem=flat.at[2],
            recv_sem=flat.at[3 + side],
            device_id=device,
            device_id_type=MESH,
        )

    @pl.when(odd == 1)
    def _():
        for d in range(1, groups):
            flat_copy(d, gram_part, gram_landed.at[d - 1], 7, samp_peer(d)).start()
        for d in range(1, groups):
            at = pl.ds(lax.rem(me + d, groups) * quota_t, quota_t)
            flat_copy(d, parts_t.at[at], landed_t.at[d - 1], 0, samp_peer(d)).start()
            g_copy(d, 0, samp_peer(d)).start()

    @pl.when(odd == 0)
    def _():
        for d in range(1, groups):
            g_copy(d, 1, {"samp": lax.rem(me + d, groups), "tile": other}).start()
        g_copy(groups, 1, {"tile": other}).start()

    def permute(k, rows):
        order = order_ref[pl.ds(k - 1, 1), :] - me * local
        for i in range(local // step):
            row = lax.broadcasted_iota(jnp.int32, (step, local), 0) + i * step
            hot = jnp.where(row == order, 1.0, 0.0).astype(BF16)
            moved[i * step : (i + 1) * step, : rows.shape[1]] = jnp.dot(
                hot, rows, preferred_element_type=F32
            ).astype(BF16)

    step = min(256, local)
    for i in range(local // step):
        at = slice(i * step, (i + 1) * step)
        rt[:, at] = t_ref[at, :].T
    cross(0, (dose - 1.0).astype(BF16))
    begin(0, 0)
    begin(0, 1)
    permute(1, jnp.concatenate([dose.astype(BF16), design[...]], axis=1))
    swap = pltpu.make_async_remote_copy(
        src_ref=gram_sum,
        dst_ref=gram_sum,
        send_sem=tile_send.at[2 * (tiles - 1)],
        recv_sem=tile_recv.at[2 * (tiles - 1)],
        device_id={"tile": other},
        device_id_type=MESH,
    )

    @pl.when(odd == 1)
    def _():
        await_all(8, gram_landed)
        total = gram_part[...]
        for d in range(1, groups):
            total = total + gram_landed[d - 1]
        gram_sum[...] = total
        swap.start()
        await_all(1, landed_t)
        total = parts_t[pl.ds(me * quota_t, quota_t)]
        for d in range(1, groups):
            total = total + landed_t[d - 1]
        mine[:quota_t] = total
        await_all(3, landed_g.at[0, pl.ds(0, groups - 1)])
        total = parts_g[pl.ds(me * quota_g, quota_g)]
        for d in range(1, groups):
            total = total + landed_g[0, d - 1]
        mine[quota_t : quota_t + quota_g] = total
        await_all(4, landed_g.at[1])
        total = landed_g[1, 0]
        for d in range(1, groups):
            total = total + landed_g[1, d]
        mine[quota_t + quota_g :] = total
        full[pair, me] = mine[...]
        for d in range(1, groups):
            flat_copy(d, mine, full.at[pair, me], 5, samp_peer(d)).start()

    rhs[...] = jnp.zeros(rhs.shape, F32)
    gram_ref[...] = jnp.zeros(gram_ref.shape, F32)
    coef[...] = jnp.zeros(coef.shape, BF16)
    half = LANES // 2

    @pl.when(odd == 0)
    def _():
        swap.wait_recv()

    for r in range(strips):
        at = slice(r % pack * 8 * strips, (r % pack + 1) * 8 * strips)
        gram_ref[8 * r : 8 * r + 8, : 8 * strips] = gram_sum[r // pack][:, at]
    gram = gram_ref[: 8 * strips, :]
    sub = lax.broadcasted_iota(jnp.int32, gram.shape, 0)
    lane = lax.broadcasted_iota(jnp.int32, gram.shape, 1)
    gram = jnp.where(lane == sub + half, 1.0, gram)
    for j in range(used):
        row = gram[j : j + 1, :] * (1.0 / gram[j : j + 1, j : j + 1])
        gram = jnp.where(sub == j, row, gram - gram[:, j : j + 1] * row)
    inverse = jnp.where(lane >= half, gram, 0.0)
    advance(0, 0, 0, True)
    advance(0, 1, 0, True)

    def spread_copy(d, q):
        return pltpu.make_async_remote_copy(
            src_ref=full.at[q],
            dst_ref=full.at[q],
            send_sem=tile_send.at[tiles - 1 + d - 1],
            recv_sem=tile_recv.at[tiles - 1 + q],
            device_id=tile_peer(d),
            device_id_type=MESH,
        )

    @pl.when(odd == 1)
    def _():
        await_all(6, full.at[0, pl.ds(0, groups - 1)])
        for d in range(1, tiles):
            spread_copy(d, pair).start()

    for q in range(pairs):

        @pl.when(jnp.logical_or(odd == 0, pair != q))
        def _():
            spread_copy(1, q).wait_recv()

    for q in range(pairs + 1):
        for c in range(n_t if q < pairs else n_g):
            at = LANES * (q * n_t + c)
            for r in range(whole):
                i = c * whole + r
                if q < pairs:
                    strip = full[q, i // quota_t, i % quota_t]
                else:
                    strip = full[pair, i // quota_g, quota_t + (1 - odd) * quota_g + i % quota_g]
                rhs[half + 8 * r : half + 8 * r + 8, at : at + LANES] = strip
            for r in range(rest):
                i, row = spot(c if q < pairs else n_t + c, r)
                to = half + 8 * whole + r
                if q < pairs:
                    strip = full[q, i // quota_g, quota_t + i % quota_g]
                else:
                    strip = full[pair, i // quota_g, quota_t + (1 - odd) * quota_g + i % quota_g]
                rhs[to : to + 1, at : at + LANES] = strip[row : row + 1, :]
    coef[: 8 * strips, :] = jnp.dot(
        inverse, rhs[...], precision=HIGHEST, preferred_element_type=F32
    ).astype(BF16)

    advance(0, 0, 1, True)
    advance(0, 1, 1, True)
    sq_t = jnp.zeros((1, traits), F32)
    for i in range(local // step):
        at = slice(i * step, (i + 1) * step)
        resid = t_ref[at, :].astype(F32) - jnp.dot(
            design[at, :], coef[:, :traits], preferred_element_type=F32
        )
        sq_t = sq_t + jnp.sum(resid * resid, axis=0, keepdims=True)
        rt[:, at] = resid.astype(BF16).T
    resid = moved[:, :width].astype(F32) - jnp.dot(
        moved[:, width:], coef[:, traits:], preferred_element_type=F32
    )
    cross(1, resid.astype(BF16))
    begin(1, 0)
    begin(1, 1)
    advance(0, 0, 2, True)
    advance(0, 1, 2, True)
    sq_g = jnp.zeros((1, width), F32)
    for i in range(local // step):
        at = slice(i * step, (i + 1) * step)
        resid = g_ref[at, :].astype(F32) - jnp.dot(
            design[at, :], coef[:, traits:], preferred_element_type=F32
        )
        sq_g = sq_g + jnp.sum(resid * resid, axis=0, keepdims=True)
        rg[at, :] = resid.astype(BF16)

    def note_squares():
        for j in range(groups):
            at = j * own // LANES * LANES
            notes[j, 0:1, :] = sq_t[:, at : at + LANES]
            for c in range(n_g):
                notes[j, 1 + c : 2 + c, :] = sq_g[:, c * LANES : (c + 1) * LANES]
            if n_g < 7:
                notes[j, 1 + n_g :, :] = jnp.zeros((7 - n_g, LANES), F32)

    def square_copy(d):
        return pltpu.make_async_remote_copy(
            src_ref=notes.at[lax.rem(me + d, groups)],
            dst_ref=squares.at[d],
            send_sem=flat.at[9],
            recv_sem=flat.at[10],
            device_id=samp_peer(d),
            device_id_type=MESH,
        )

    note_squares()
    squares[0] = notes[me]
    for d in range(1, groups):
        square_copy(d).start()

    lead = pl.multiple_of(me * own // LANES * LANES, LANES)
    shift = pl.multiple_of(lax.rem(me * own, LANES), 8)

    def correct():
        gram = gram_ref[...]
        lane = lax.broadcasted_iota(jnp.int32, gram.shape, 1)
        gram = jnp.where(lane < half, gram, 0.0)
        coef_g = coef[:, traits:].astype(F32)
        miss = rhs[half:, traits:] - jnp.dot(
            gram, coef_g, precision=HIGHEST, preferred_element_type=F32
        )
        sub = lax.broadcasted_iota(jnp.int32, (half, width), 0)
        fit = coef_g[:half] - jnp.where(sub == used - 1, 1.0, 0.0)
        left = jnp.concatenate(
            [rhs[half:, pl.ds(lead, LANES)], coef[:half, pl.ds(lead, LANES)].astype(F32)], axis=0
        )
        column[...] = left.T
        fix[...] = jnp.dot(
            column[pl.ds(shift, own), :],
            jnp.concatenate([fit, miss], axis=0),
            precision=HIGHEST,
            preferred_element_type=F32,
        )

    correct()

    peaks[0] = jnp.zeros(peaks.shape[1:], F32)

    def scale():
        total = squares[0]
        await_all(10, squares.at[pl.ds(1, groups - 1)])
        for d in range(1, groups):
            total = total + squares[d]
        gain = lax.rsqrt(total / samples + epsilon)
        factor = math.sqrt(samples - used - 1) / samples
        for c in range(n_g):
            gain_g[:, c * LANES : (c + 1) * LANES] = jnp.broadcast_to(
                gain[1 + c : 2 + c, :], (8, LANES)
            )
        column[...] = jnp.broadcast_to(gain.T[:, :1] * factor, column.shape)

    def peak_of(k):
        gain_t = column[pl.ds(shift, own), :]
        peak = jnp.max(jnp.abs(found[k] * gain_g[:1, :]), axis=1, keepdims=True) * gain_t
        pos = lax.broadcasted_iota(jnp.int32, peak.shape, 1)
        peaks[0] = jnp.where(pos == k - 1, peak, peaks[0])

    def turn(t, carry):
        for stage in range(3, bits):

            @pl.when(t == stage - 1)
            def _():
                advance(0, 0, stage, True)
                advance(0, 1, stage, True)

        fresh = jnp.logical_and(t > 1, t < turns)

        @pl.when(fresh)
        def _():
            begin(t, 0)

        @pl.when(t + 1 < turns)
        def _():
            permute(t + 1, rg[...])
            cross(t + 1, moved[:, :width])

        for part in range(2):
            if part == 1:

                @pl.when(fresh)
                def _():
                    begin(t, 1)

            for stage in range(bits):
                back = part - 1 - stage
                k = t + back // 2

                @pl.when(jnp.logical_and(k > 0, k < turns))
                def _():
                    advance(k, back % 2, stage)

        @pl.when(t == 2)
        def _():
            scale()

        k = t - (bits + 1) // 2

        @pl.when(k == 0)
        def _():
            score_ref[...] = (
                (found[0] - fix[...]) * gain_g[:1, :] * column[pl.ds(shift, own), :][:, :1]
            )

        @pl.when(k > 0)
        def _():
            peak_of(k)

        return carry

    lax.fori_loop(1, turns + (bits + 1) // 2, turn, 0)
    crossed = [
        pltpu.make_async_remote_copy(
            src_ref=peaks.at[0],
            dst_ref=peaks.at[d],
            send_sem=tile_send.at[d - 1],
            recv_sem=tile_recv.at[d - 1],
            device_id=tile_peer(d),
            device_id_type=MESH,
        )
        for d in range(1, tiles)
    ]
    for copy in crossed:
        copy.start()

    @pl.when(odd == 1)
    def _():
        for d in range(1, tiles):
            spread_copy(d, pair).wait_send()
        swap.wait_send()
        await_all(0, landed_t)
        await_all(2, landed_g.at[0, pl.ds(0, groups - 1)])
        await_all(5, full.at[0, pl.ds(0, groups - 1)])
        await_all(7, gram_landed)

    @pl.when(odd == 0)
    def _():
        await_all(2, landed_g.at[1])

    await_all(9, squares.at[pl.ds(1, groups - 1)])
    for p in range(n_parts):
        for stage in range(len(areas[p][0])):
            for copy in copies(turns - 1, p, stage):
                copy.wait_send()
    top = peaks[0]
    for d in range(1, tiles):
        crossed[d - 1].wait()
        top = jnp.maximum(top, peaks[d])
    peak_ref[...] = top.T[: turns - 1]


def shards(traits, covariates, genotypes, shuffles):
    groups, tiles = lax.axis_size("samp"), lax.axis_size("tile")
    bits = groups.bit_length() - 1
    turns = shuffles.shape[0] + 1
    local, n_traits = traits.shape
    width = genotypes.shape[1]
    used = covariates.shape[1] + 1
    own = n_traits // groups
    areas = parts_of(bits, own, width)
    bufs = []
    for order, part_rows, part_lanes in areas:
        size = (part_rows.stop - part_rows.start, part_lanes.stop - part_lanes.start)
        lot = groups
        for some in order:
            n = 2 ** len(some)
            lot //= n
            bufs.append(pltpu.VMEM((turns, n, lot) + size, F32))
            bufs.append(pltpu.VMEM((turns, n - 1, lot) + size, F32))
    pairs, whole, rest = tiles // 2, used // 8, used % 8
    n_t, n_g, strips = n_traits // pairs // LANES, width // LANES, -(-used // 8)
    quota_t = -(-n_t * whole // groups)
    quota_g = -(-(n_g * whole + -(-(n_t + n_g) * rest // 8)) // groups)
    quota = quota_t + 2 * quota_g
    lots = -(-strips // (LANES // (8 * strips)))
    vmem = pl.BlockSpec(memory_space=pltpu.VMEM)
    sems = pltpu.SemaphoreType.DMA((2, len(areas), bits + 1))
    pair = pltpu.SemaphoreType.DMA((2 * tiles - 1,))
    return pl.pallas_call(
        functools.partial(scan_kernel, groups, tiles, local * groups, used, areas),
        out_shape=(
            pltpu.VMEM((own, width), F32),
            pltpu.VMEM((turns - 1, own), F32),
        ),
        in_specs=[pl.BlockSpec(memory_space=pl.ANY)] * 4,
        out_specs=(vmem, vmem),
        scratch_shapes=[
            pltpu.VMEM((local, n_traits), BF16),
            pltpu.VMEM((used - 1, local), BF16),
            pltpu.VMEM((local, width), jnp.int32),
            pltpu.VMEM((turns - 1, local), jnp.int32),
            pltpu.SemaphoreType.DMA((10,)),
            pltpu.VMEM((local, LANES), BF16),
            pltpu.VMEM((groups * quota_t, 8, LANES), F32),
            pltpu.VMEM((groups * quota_g, 8, LANES), F32),
            pltpu.VMEM((groups - 1, quota_t, 8, LANES), F32),
            pltpu.VMEM((2, groups, quota_g, 8, LANES), F32),
            pltpu.VMEM((quota, 8, LANES), F32),
            pltpu.VMEM((pairs, groups, quota, 8, LANES), F32),
            pltpu.VMEM((LANES, n_traits + width), F32),
            pltpu.VMEM((LANES, n_traits + width), BF16),
            pltpu.VMEM((n_traits, local), BF16),
            pltpu.VMEM((local, width), BF16),
            pltpu.VMEM((local, width + LANES), BF16),
            pltpu.VMEM((turns, own, width), F32),
            pltpu.VMEM((own, width), F32),
            pltpu.VMEM((lots, 8, LANES), F32),
            pltpu.VMEM((groups - 1, lots, 8, LANES), F32),
            pltpu.VMEM((lots, 8, LANES), F32),
            pltpu.VMEM((LANES // 2, LANES), F32),
            pltpu.VMEM((groups, 8, LANES), F32),
            pltpu.VMEM((groups, 8, LANES), F32),
            pltpu.VMEM((LANES, LANES), F32),
            pltpu.VMEM((8, width), F32),
            pltpu.VMEM((tiles, own, LANES), F32),
            pltpu.SemaphoreType.DMA((11,)),
            pair,
            pair,
            sems,
            sems,
            *bufs,
        ],
        compiler_params=pltpu.CompilerParams(
            collective_id=0, has_side_effects=True, vmem_limit_bytes=60 * 1024 * 1024
        ),
        name="scan",
    )(traits, covariates.T, genotypes, shuffles)


def solution(mesh):
    placed = (P("samp", None), P("samp", None), P("samp", "tile"), P(None, "samp"))
    return jax.shard_map(
        shards,
        mesh=mesh,
        in_specs=placed,
        out_specs=(P("samp", "tile"), P(None, "samp")),
        check_vma=False,
    )
```

```python
import functools
import math

import jax
import jax.numpy as jnp
from jax import lax
from jax.experimental import pallas as pl
from jax.experimental.pallas import tpu as pltpu
from jax.sharding import PartitionSpec as P

MESH = pl.DeviceIdType.MESH
LANES = 128
F32, BF16 = jnp.float32, jnp.bfloat16
HIGHEST = lax.Precision.HIGHEST
epsilon = 1e-05


def parts_of(bits, own, width):
    cut, half = own - max(8, own // 32 * 8), width // 2
    mid = (cut // 8 + 1) // 2 * 8
    ones = tuple((bit,) for bit in range(bits))
    far = ones[2:-2] + ((bits - 2, bits - 1),)
    x_first, y_first = ones[:2] + far, ones[1::-1] + far
    return (
        (x_first, slice(0, mid), slice(0, half)),
        (y_first, slice(0, mid), slice(half, width)),
        (ones[2:] + ones[:2], slice(cut, own), slice(0, half)),
        (ones[2::-1] + ones[3:], slice(cut, own), slice(half, width)),
        (x_first, slice(mid, cut), slice(0, half)),
        (y_first, slice(mid, cut), slice(half, width)),
    )


HALVES = ((0, 1, 2, 3), (4, 5))


def place_of(order, g):
    at = [g >> some[0] & 2 ** len(some) - 1 for some in order]
    rest = 0
    for digit, some in zip(at[1:], order[1:]):
        rest = 2 ** len(some) * rest + digit
    return at[0], rest


def scan_kernel(
    groups, tiles, samples, used, areas, t_hbm, c_hbm, g_hbm, order_hbm, score_ref, peak_ref,
    t_ref, c_ref, g_ref, order_ref, load, design, parts_t, parts_g, landed_t, landed_g, mine, full, rhs, coef, rt, rg,
    moved, found, fix, gram_part, gram_landed, gram_sum, gram_ref, notes, squares, column, gain_g,
    peaks, flat, tile_send, tile_recv, send, recv, *bufs
):
    me = lax.axis_index("samp")
    my_tile = lax.axis_index("tile")
    turns, width, n_parts = found.shape[0], found.shape[2], len(areas)
    bits = groups.bit_length() - 1
    local, traits = t_ref.shape
    own = traits // groups
    pairs = tiles // 2
    share = traits // pairs
    quota_t, quota_g = parts_t.shape[0] // groups, parts_g.shape[0] // groups
    odd, pair = lax.rem(my_tile, 2), my_tile // 2
    other = my_tile + 1 - 2 * odd

    def samp_peer(d):
        return {"samp": lax.rem(me + d, groups)}

    def tile_peer(d):
        return {"tile": lax.rem(my_tile + d, tiles)}

    barrier = pltpu.get_barrier_semaphore()
    for d in range(1, groups):
        pl.semaphore_signal(barrier, inc=1, device_id=samp_peer(d), device_id_type=MESH)
    for d in range(1, tiles):
        pl.semaphore_signal(barrier, inc=1, device_id=tile_peer(d), device_id_type=MESH)
    for d in range(1, groups):
        pl.semaphore_signal(
            barrier,
            inc=1,
            device_id={"samp": lax.rem(me + d, groups), "tile": other},
            device_id_type=MESH,
        )
    chunk = local // 4
    pieces = [(c_hbm, c_ref)]
    for i in range(4):
        at = pl.ds(i * chunk, chunk)
        pieces.append((g_hbm.at[at], g_ref.at[at]))
        pieces.append((t_hbm.at[at], t_ref.at[at]))
    pieces.append((order_hbm, order_ref))
    loads = [pltpu.make_async_copy(a, b, load.at[i]) for i, (a, b) in enumerate(pieces)]
    for copy in loads:
        copy.start()
    for copy in loads:
        copy.wait()

    lane = lax.broadcasted_iota(jnp.int32, (LANES - used + 1, local), 0)
    design_t = jnp.concatenate(
        [c_ref[...].astype(F32), jnp.where(lane == 0, 1.0, 0.0)], axis=0
    )
    design[...] = design_t.T.astype(BF16)
    design_t = design_t[: -(-used // 16) * 16].astype(BF16)
    n_t, n_g = share // LANES, width // LANES
    whole, rest = used // 8, used % 8
    strips = -(-used // 8)

    def spot(c, r):
        at = c * rest + r
        return n_g * whole + at // 8, at % 8

    for i in range(n_g * whole, parts_g.shape[0]):
        parts_g[i] = jnp.zeros((8, LANES), F32)
    dose = g_ref[...].astype(F32)

    def put(block, parts, first):
        for c in range(block.shape[1] // LANES):
            at = slice(LANES * c, LANES * c + LANES)
            for r in range(whole):
                parts[c * whole + r] = block[8 * r : 8 * r + 8, at]
            for r in range(rest):
                slot, row = spot(first + c, r)
                parts_g[slot, row : row + 1, :] = block[8 * whole + r : 8 * whole + r + 1, at]

    put(jnp.dot(design_t, dose.astype(BF16), preferred_element_type=F32), parts_g, n_t)

    @pl.when(odd == 1)
    def _():
        block = t_ref[:, pl.ds(pl.multiple_of(pair * share, LANES), share)]
        put(jnp.dot(design_t, block, preferred_element_type=F32), parts_t, 0)
        for i in range(n_t * whole, parts_t.shape[0]):
            parts_t[i] = jnp.zeros((8, LANES), F32)

    gram = jnp.dot(design_t, design[...], preferred_element_type=F32)
    gram_part[...] = jnp.zeros(gram_part.shape, F32)
    pack = LANES // (8 * strips)
    for r in range(strips):
        at = slice(r % pack * 8 * strips, (r % pack + 1) * 8 * strips)
        gram_part[r // pack, :, at] = gram[8 * r : 8 * r + 8, : 8 * strips]

    def await_all(sem, like):
        pltpu.make_async_copy(like, like, flat.at[sem]).wait()

    starts = [sum(2 * len(area[0]) for area in areas[:p]) for p in range(n_parts)]

    places = [sum(len(area[0]) for area in areas[:p]) for p in range(n_parts)]

    def source(p, stage):
        return bufs[starts[p] + 2 * stage]

    def target(p, stage):
        return bufs[starts[p] + 2 * stage + 1]

    def digit(p, stage):
        some = areas[p][0][stage]
        return lax.rem(me // 2 ** some[0], 2 ** len(some)), 2 ** len(some), 2 ** some[0]

    def copies(k, p, stage):
        mine, n, far = digit(p, stage)
        at = lax.rem(k, 2), places[p] + stage
        out = []
        for d in range(1, n):
            other = lax.rem(mine + d, n)
            out.append(
                pltpu.make_async_remote_copy(
                    src_ref=source(p, stage).at[k, other],
                    dst_ref=target(p, stage).at[k, d - 1],
                    send_sem=send.at[at],
                    recv_sem=recv.at[at],
                    device_id={"samp": me + (other - mine) * far},
                    device_id_type=MESH,
                )
            )
        return out

    def await_stage(k, p, stage, sems, like):
        sem = sems.at[lax.rem(k, 2), places[p] + stage]
        pltpu.make_async_copy(like, like, sem).wait()

    def await_sent(k, p, stage):
        n = digit(p, stage)[1]
        await_stage(k, p, stage, send, source(p, stage).at[k, pl.ds(0, n - 1)])

    def begin(k, part):
        for p in HALVES[part]:
            for copy in copies(k, p, 0):
                copy.start()

    def advance(k, part, stage, first=False):
        for p in HALVES[part]:
            if stage >= len(areas[p][0]):
                continue
            await_stage(k, p, stage, recv, target(p, stage).at[k])
            if not first:
                await_sent(k - 1, p, stage)
            mine, n, _ = digit(p, stage)
            total = source(p, stage)[k, mine]
            for d in range(1, n):
                total = total + target(p, stage)[k, d - 1]
            if stage < len(areas[p][0]) - 1:
                source(p, stage + 1)[k] = total.reshape(source(p, stage + 1).shape[1:])
                for copy in copies(k, p, stage + 1):
                    copy.start()
            else:
                found[k, areas[p][1], areas[p][2]] = total[0]

    def cross(k, right):
        batch = max(groups // 4, 1)
        for q in range(groups // batch):
            rows = batch * own
            block = jnp.dot(
                rt[q * rows : (q + 1) * rows, :], right, preferred_element_type=F32
            )
            for i in range(batch):
                for p in range(n_parts):
                    order, part_rows, part_lanes = areas[p]
                    lead, other = place_of(order, q * batch + i)
                    source(p, 0)[k, lead, other] = block[i * own : (i + 1) * own][
                        part_rows, part_lanes
                    ]

    pl.semaphore_wait(barrier, 2 * (groups - 1) + tiles - 1)

    def flat_copy(d, source, target, sem, device):
        return pltpu.make_async_remote_copy(
            src_ref=source,
            dst_ref=target,
            send_sem=flat.at[sem],
            recv_sem=flat.at[sem + 1],
            device_id=device,
            device_id_type=MESH,
        )

    def g_copy(d, side, device):
        at = pl.ds(lax.rem(me + d, groups) * quota_g, quota_g)
        return pltpu.make_async_remote_copy(
            src_ref=parts_g.at[at],
            dst_ref=landed_g.at[side, d - 1],
            send_sem=flat.at[2],
            recv_sem=flat.at[3 + side],
            device_id=device,
            device_id_type=MESH,
        )

    @pl.when(odd == 1)
    def _():
        for d in range(1, groups):
            flat_copy(d, gram_part, gram_landed.at[d - 1], 7, samp_peer(d)).start()
        for d in range(1, groups):
            at = pl.ds(lax.rem(me + d, groups) * quota_t, quota_t)
            flat_copy(d, parts_t.at[at], landed_t.at[d - 1], 0, samp_peer(d)).start()
            g_copy(d, 0, samp_peer(d)).start()

    @pl.when(odd == 0)
    def _():
        for d in range(1, groups):
            g_copy(d, 1, {"samp": lax.rem(me + d, groups), "tile": other}).start()
        g_copy(groups, 1, {"tile": other}).start()

    def permute(k, rows):
        order = order_ref[pl.ds(k - 1, 1), :] - me * local
        for i in range(local // step):
            row = lax.broadcasted_iota(jnp.int32, (step, local), 0) + i * step
            hot = jnp.where(row == order, 1.0, 0.0).astype(BF16)
            moved[i * step : (i + 1) * step, : rows.shape[1]] = jnp.dot(
                hot, rows, preferred_element_type=F32
            ).astype(BF16)

    step = min(256, local)
    for i in range(local // step):
        at = slice(i * step, (i + 1) * step)
        rt[:, at] = t_ref[at, :].T
    cross(0, (dose - 1.0).astype(BF16))
    begin(0, 0)
    begin(0, 1)
    permute(1, jnp.concatenate([dose.astype(BF16), design[...]], axis=1))
    swap = pltpu.make_async_remote_copy(
        src_ref=gram_sum,
        dst_ref=gram_sum,
        send_sem=tile_send.at[2 * (tiles - 1)],
        recv_sem=tile_recv.at[2 * (tiles - 1)],
        device_id={"tile": other},
        device_id_type=MESH,
    )

    @pl.when(odd == 1)
    def _():
        await_all(8, gram_landed)
        total = gram_part[...]
        for d in range(1, groups):
            total = total + gram_landed[d - 1]
        gram_sum[...] = total
        swap.start()
        await_all(1, landed_t)
        total = parts_t[pl.ds(me * quota_t, quota_t)]
        for d in range(1, groups):
            total = total + landed_t[d - 1]
        mine[:quota_t] = total
        await_all(3, landed_g.at[0, pl.ds(0, groups - 1)])
        total = parts_g[pl.ds(me * quota_g, quota_g)]
        for d in range(1, groups):
            total = total + landed_g[0, d - 1]
        mine[quota_t : quota_t + quota_g] = total
        await_all(4, landed_g.at[1])
        total = landed_g[1, 0]
        for d in range(1, groups):
            total = total + landed_g[1, d]
        mine[quota_t + quota_g :] = total
        full[pair, me] = mine[...]
        for d in range(1, groups):
            flat_copy(d, mine, full.at[pair, me], 5, samp_peer(d)).start()

    rhs[...] = jnp.zeros(rhs.shape, F32)
    gram_ref[...] = jnp.zeros(gram_ref.shape, F32)
    coef[...] = jnp.zeros(coef.shape, BF16)
    half = LANES // 2

    @pl.when(odd == 0)
    def _():
        swap.wait_recv()

    for r in range(strips):
        at = slice(r % pack * 8 * strips, (r % pack + 1) * 8 * strips)
        gram_ref[8 * r : 8 * r + 8, : 8 * strips] = gram_sum[r // pack][:, at]
    gram = gram_ref[: 8 * strips, :]
    sub = lax.broadcasted_iota(jnp.int32, gram.shape, 0)
    lane = lax.broadcasted_iota(jnp.int32, gram.shape, 1)
    gram = jnp.where(lane == sub + half, 1.0, gram)
    for j in range(used):
        row = gram[j : j + 1, :] * (1.0 / gram[j : j + 1, j : j + 1])
        gram = jnp.where(sub == j, row, gram - gram[:, j : j + 1] * row)
    inverse = jnp.where(lane >= half, gram, 0.0)
    advance(0, 0, 0, True)
    advance(0, 1, 0, True)

    def spread_copy(d, q):
        return pltpu.make_async_remote_copy(
            src_ref=full.at[q],
            dst_ref=full.at[q],
            send_sem=tile_send.at[tiles - 1 + d - 1],
            recv_sem=tile_recv.at[tiles - 1 + q],
            device_id=tile_peer(d),
            device_id_type=MESH,
        )

    @pl.when(odd == 1)
    def _():
        await_all(6, full.at[0, pl.ds(0, groups - 1)])
        for d in range(1, tiles):
            spread_copy(d, pair).start()

    for q in range(pairs):

        @pl.when(jnp.logical_or(odd == 0, pair != q))
        def _():
            spread_copy(1, q).wait_recv()

    for q in range(pairs + 1):
        for c in range(n_t if q < pairs else n_g):
            at = LANES * (q * n_t + c)
            for r in range(whole):
                i = c * whole + r
                if q < pairs:
                    strip = full[q, i // quota_t, i % quota_t]
                else:
                    strip = full[pair, i // quota_g, quota_t + (1 - odd) * quota_g + i % quota_g]
                rhs[half + 8 * r : half + 8 * r + 8, at : at + LANES] = strip
            for r in range(rest):
                i, row = spot(c if q < pairs else n_t + c, r)
                to = half + 8 * whole + r
                if q < pairs:
                    strip = full[q, i // quota_g, quota_t + i % quota_g]
                else:
                    strip = full[pair, i // quota_g, quota_t + (1 - odd) * quota_g + i % quota_g]
                rhs[to : to + 1, at : at + LANES] = strip[row : row + 1, :]
    coef[: 8 * strips, :] = jnp.dot(
        inverse, rhs[...], precision=HIGHEST, preferred_element_type=F32
    ).astype(BF16)

    advance(0, 0, 1, True)
    advance(0, 1, 1, True)
    sq_t = jnp.zeros((1, traits), F32)
    for i in range(local // step):
        at = slice(i * step, (i + 1) * step)
        resid = t_ref[at, :].astype(F32) - jnp.dot(
            design[at, :], coef[:, :traits], preferred_element_type=F32
        )
        sq_t = sq_t + jnp.sum(resid * resid, axis=0, keepdims=True)
        rt[:, at] = resid.astype(BF16).T
    resid = moved[:, :width].astype(F32) - jnp.dot(
        moved[:, width:], coef[:, traits:], preferred_element_type=F32
    )
    cross(1, resid.astype(BF16))
    begin(1, 0)
    begin(1, 1)
    advance(0, 0, 2, True)
    advance(0, 1, 2, True)
    sq_g = jnp.zeros((1, width), F32)
    for i in range(local // step):
        at = slice(i * step, (i + 1) * step)
        resid = g_ref[at, :].astype(F32) - jnp.dot(
            design[at, :], coef[:, traits:], preferred_element_type=F32
        )
        sq_g = sq_g + jnp.sum(resid * resid, axis=0, keepdims=True)
        rg[at, :] = resid.astype(BF16)

    def note_squares():
        for j in range(groups):
            at = j * own // LANES * LANES
            notes[j, 0:1, :] = sq_t[:, at : at + LANES]
            for c in range(n_g):
                notes[j, 1 + c : 2 + c, :] = sq_g[:, c * LANES : (c + 1) * LANES]
            if n_g < 7:
                notes[j, 1 + n_g :, :] = jnp.zeros((7 - n_g, LANES), F32)

    def square_copy(d):
        return pltpu.make_async_remote_copy(
            src_ref=notes.at[lax.rem(me + d, groups)],
            dst_ref=squares.at[d],
            send_sem=flat.at[9],
            recv_sem=flat.at[10],
            device_id=samp_peer(d),
            device_id_type=MESH,
        )

    note_squares()
    squares[0] = notes[me]
    for d in range(1, groups):
        square_copy(d).start()

    lead = pl.multiple_of(me * own // LANES * LANES, LANES)
    shift = pl.multiple_of(lax.rem(me * own, LANES), 8)

    def correct():
        gram = gram_ref[...]
        lane = lax.broadcasted_iota(jnp.int32, gram.shape, 1)
        gram = jnp.where(lane < half, gram, 0.0)
        coef_g = coef[:, traits:].astype(F32)
        miss = rhs[half:, traits:] - jnp.dot(
            gram, coef_g, precision=HIGHEST, preferred_element_type=F32
        )
        sub = lax.broadcasted_iota(jnp.int32, (half, width), 0)
        fit = coef_g[:half] - jnp.where(sub == used - 1, 1.0, 0.0)
        left = jnp.concatenate(
            [rhs[half:, pl.ds(lead, LANES)], coef[:half, pl.ds(lead, LANES)].astype(F32)], axis=0
        )
        column[...] = left.T
        fix[...] = jnp.dot(
            column[pl.ds(shift, own), :],
            jnp.concatenate([fit, miss], axis=0),
            precision=HIGHEST,
            preferred_element_type=F32,
        )

    correct()

    peaks[0] = jnp.zeros(peaks.shape[1:], F32)

    def scale():
        total = squares[0]
        await_all(10, squares.at[pl.ds(1, groups - 1)])
        for d in range(1, groups):
            total = total + squares[d]
        gain = lax.rsqrt(total / samples + epsilon)
        factor = math.sqrt(samples - used - 1) / samples
        for c in range(n_g):
            gain_g[:, c * LANES : (c + 1) * LANES] = jnp.broadcast_to(
                gain[1 + c : 2 + c, :], (8, LANES)
            )
        column[...] = jnp.broadcast_to(gain.T[:, :1] * factor, column.shape)

    def peak_of(k):
        gain_t = column[pl.ds(shift, own), :]
        peak = jnp.max(jnp.abs(found[k] * gain_g[:1, :]), axis=1, keepdims=True) * gain_t
        pos = lax.broadcasted_iota(jnp.int32, peak.shape, 1)
        peaks[0] = jnp.where(pos == k - 1, peak, peaks[0])

    def turn(t, carry):
        for stage in range(3, bits):

            @pl.when(t == stage - 1)
            def _():
                advance(0, 0, stage, True)
                advance(0, 1, stage, True)

        fresh = jnp.logical_and(t > 1, t < turns)

        @pl.when(fresh)
        def _():
            begin(t, 0)

        @pl.when(t + 1 < turns)
        def _():
            permute(t + 1, rg[...])
            cross(t + 1, moved[:, :width])

        for part in range(2):
            if part == 1:

                @pl.when(fresh)
                def _():
                    begin(t, 1)

            for stage in range(bits):
                back = part - 1 - stage
                k = t + back // 2

                @pl.when(jnp.logical_and(k > 0, k < turns))
                def _():
                    advance(k, back % 2, stage)

        @pl.when(t == 2)
        def _():
            scale()

        k = t - (bits + 1) // 2

        @pl.when(k == 0)
        def _():
            score_ref[...] = (
                (found[0] - fix[...]) * gain_g[:1, :] * column[pl.ds(shift, own), :][:, :1]
            )

        @pl.when(k > 0)
        def _():
            peak_of(k)

        return carry

    lax.fori_loop(1, turns + (bits + 1) // 2, turn, 0)
    crossed = [
        pltpu.make_async_remote_copy(
            src_ref=peaks.at[0],
            dst_ref=peaks.at[d],
            send_sem=tile_send.at[d - 1],
            recv_sem=tile_recv.at[d - 1],
            device_id=tile_peer(d),
            device_id_type=MESH,
        )
        for d in range(1, tiles)
    ]
    for copy in crossed:
        copy.start()

    @pl.when(odd == 1)
    def _():
        for d in range(1, tiles):
            spread_copy(d, pair).wait_send()
        swap.wait_send()
        await_all(0, landed_t)
        await_all(2, landed_g.at[0, pl.ds(0, groups - 1)])
        await_all(5, full.at[0, pl.ds(0, groups - 1)])
        await_all(7, gram_landed)

    @pl.when(odd == 0)
    def _():
        await_all(2, landed_g.at[1])

    await_all(9, squares.at[pl.ds(1, groups - 1)])
    for p in range(n_parts):
        for stage in range(len(areas[p][0])):
            await_sent(turns - 1, p, stage)
    top = peaks[0]
    for d in range(1, tiles):
        crossed[d - 1].wait()
        top = jnp.maximum(top, peaks[d])
    peak_ref[...] = top.T[: turns - 1]


def shards(traits, covariates, genotypes, shuffles):
    groups, tiles = lax.axis_size("samp"), lax.axis_size("tile")
    bits = groups.bit_length() - 1
    turns = shuffles.shape[0] + 1
    local, n_traits = traits.shape
    width = genotypes.shape[1]
    used = covariates.shape[1] + 1
    own = n_traits // groups
    areas = parts_of(bits, own, width)
    bufs = []
    for order, part_rows, part_lanes in areas:
        size = (part_rows.stop - part_rows.start, part_lanes.stop - part_lanes.start)
        lot = groups
        for some in order:
            n = 2 ** len(some)
            lot //= n
            bufs.append(pltpu.VMEM((turns, n, lot) + size, F32))
            bufs.append(pltpu.VMEM((turns, n - 1, lot) + size, F32))
    pairs, whole, rest = tiles // 2, used // 8, used % 8
    n_t, n_g, strips = n_traits // pairs // LANES, width // LANES, -(-used // 8)
    quota_t = -(-n_t * whole // groups)
    quota_g = -(-(n_g * whole + -(-(n_t + n_g) * rest // 8)) // groups)
    quota = quota_t + 2 * quota_g
    lots = -(-strips // (LANES // (8 * strips)))
    vmem = pl.BlockSpec(memory_space=pltpu.VMEM)
    sems = pltpu.SemaphoreType.DMA((2, sum(len(area[0]) for area in areas)))
    pair = pltpu.SemaphoreType.DMA((2 * tiles - 1,))
    return pl.pallas_call(
        functools.partial(scan_kernel, groups, tiles, local * groups, used, areas),
        out_shape=(
            pltpu.VMEM((own, width), F32),
            pltpu.VMEM((turns - 1, own), F32),
        ),
        in_specs=[pl.BlockSpec(memory_space=pl.ANY)] * 4,
        out_specs=(vmem, vmem),
        scratch_shapes=[
            pltpu.VMEM((local, n_traits), BF16),
            pltpu.VMEM((used - 1, local), BF16),
            pltpu.VMEM((local, width), jnp.int32),
            pltpu.VMEM((turns - 1, local), jnp.int32),
            pltpu.SemaphoreType.DMA((10,)),
            pltpu.VMEM((local, LANES), BF16),
            pltpu.VMEM((groups * quota_t, 8, LANES), F32),
            pltpu.VMEM((groups * quota_g, 8, LANES), F32),
            pltpu.VMEM((groups - 1, quota_t, 8, LANES), F32),
            pltpu.VMEM((2, groups, quota_g, 8, LANES), F32),
            pltpu.VMEM((quota, 8, LANES), F32),
            pltpu.VMEM((pairs, groups, quota, 8, LANES), F32),
            pltpu.VMEM((LANES, n_traits + width), F32),
            pltpu.VMEM((LANES, n_traits + width), BF16),
            pltpu.VMEM((n_traits, local), BF16),
            pltpu.VMEM((local, width), BF16),
            pltpu.VMEM((local, width + LANES), BF16),
            pltpu.VMEM((turns, own, width), F32),
            pltpu.VMEM((own, width), F32),
            pltpu.VMEM((lots, 8, LANES), F32),
            pltpu.VMEM((groups - 1, lots, 8, LANES), F32),
            pltpu.VMEM((lots, 8, LANES), F32),
            pltpu.VMEM((LANES // 2, LANES), F32),
            pltpu.VMEM((groups, 8, LANES), F32),
            pltpu.VMEM((groups, 8, LANES), F32),
            pltpu.VMEM((LANES, LANES), F32),
            pltpu.VMEM((8, width), F32),
            pltpu.VMEM((tiles, own, LANES), F32),
            pltpu.SemaphoreType.DMA((11,)),
            pair,
            pair,
            sems,
            sems,
            *bufs,
        ],
        compiler_params=pltpu.CompilerParams(
            collective_id=0, has_side_effects=True, vmem_limit_bytes=60 * 1024 * 1024
        ),
        name="scan",
    )(traits, covariates.T, genotypes, shuffles)


def solution(mesh):
    placed = (P("samp", None), P("samp", None), P("samp", "tile"), P(None, "samp"))
    return jax.shard_map(
        shards,
        mesh=mesh,
        in_specs=placed,
        out_specs=(P("samp", "tile"), P(None, "samp")),
        check_vma=False,
    )
```

```python
import functools
import math

import jax
import jax.numpy as jnp
from jax import lax
from jax.experimental import pallas as pl
from jax.experimental.pallas import tpu as pltpu
from jax.sharding import PartitionSpec as P

MESH = pl.DeviceIdType.MESH
LANES = 128
F32, BF16 = jnp.float32, jnp.bfloat16
HIGHEST = lax.Precision.HIGHEST
epsilon = 1e-05


def parts_of(bits, own, width):
    cut, half = own - max(8, own // 32 * 8), width // 2
    mid = (cut // 8 + 1) // 2 * 8
    ones = tuple((bit,) for bit in range(bits))
    far = ones[2:-2] + ((bits - 2, bits - 1),)
    x_first, y_first = ones[:2] + far, ones[1::-1] + far
    return (
        (x_first, slice(0, mid), slice(0, half)),
        (y_first, slice(0, mid), slice(half, width)),
        (ones[2:] + ones[1::-1], slice(cut, own), slice(0, half)),
        ((ones[2],) + ones[:2] + ones[3:], slice(cut, own), slice(half, width)),
        (x_first, slice(mid, cut), slice(0, half)),
        (y_first, slice(mid, cut), slice(half, width)),
    )


HALVES = ((0, 1, 2, 3), (4, 5))


def place_of(order, g):
    at = [g >> some[0] & 2 ** len(some) - 1 for some in order]
    rest = 0
    for digit, some in zip(at[1:], order[1:]):
        rest = 2 ** len(some) * rest + digit
    return at[0], rest


def scan_kernel(
    groups, tiles, samples, used, areas, t_hbm, c_hbm, g_hbm, order_hbm, score_ref, peak_ref,
    t_ref, c_ref, g_ref, order_ref, load, design, parts_t, parts_g, landed_t, landed_g, mine, full, rhs, coef, rt, rg,
    moved, found, fix, gram_part, gram_landed, gram_sum, gram_ref, notes, squares, column, gain_g,
    peaks, flat, tile_send, tile_recv, send, recv, *bufs
):
    me = lax.axis_index("samp")
    my_tile = lax.axis_index("tile")
    turns, width, n_parts = found.shape[0], found.shape[2], len(areas)
    bits = groups.bit_length() - 1
    local, traits = t_ref.shape
    own = traits // groups
    pairs = tiles // 2
    share = traits // pairs
    quota_t, quota_g = parts_t.shape[0] // groups, parts_g.shape[0] // groups
    odd, pair = lax.rem(my_tile, 2), my_tile // 2
    other = my_tile + 1 - 2 * odd

    def samp_peer(d):
        return {"samp": lax.rem(me + d, groups)}

    def tile_peer(d):
        return {"tile": lax.rem(my_tile + d, tiles)}

    barrier = pltpu.get_barrier_semaphore()
    for d in range(1, groups):
        pl.semaphore_signal(barrier, inc=1, device_id=samp_peer(d), device_id_type=MESH)
    for d in range(1, tiles):
        pl.semaphore_signal(barrier, inc=1, device_id=tile_peer(d), device_id_type=MESH)
    for d in range(1, groups):
        pl.semaphore_signal(
            barrier,
            inc=1,
            device_id={"samp": lax.rem(me + d, groups), "tile": other},
            device_id_type=MESH,
        )
    chunk = local // 4
    pieces = [(c_hbm, c_ref)]
    for i in range(4):
        at = pl.ds(i * chunk, chunk)
        pieces.append((g_hbm.at[at], g_ref.at[at]))
        pieces.append((t_hbm.at[at], t_ref.at[at]))
    pieces.append((order_hbm, order_ref))
    loads = [pltpu.make_async_copy(a, b, load.at[i]) for i, (a, b) in enumerate(pieces)]
    for copy in loads:
        copy.start()
    for copy in loads:
        copy.wait()

    lane = lax.broadcasted_iota(jnp.int32, (LANES - used + 1, local), 0)
    design_t = jnp.concatenate(
        [c_ref[...].astype(F32), jnp.where(lane == 0, 1.0, 0.0)], axis=0
    )
    design[...] = design_t.T.astype(BF16)
    design_t = design_t[: -(-used // 16) * 16].astype(BF16)
    n_t, n_g = share // LANES, width // LANES
    whole, rest = used // 8, used % 8
    strips = -(-used // 8)

    def spot(c, r):
        at = c * rest + r
        return n_g * whole + at // 8, at % 8

    for i in range(n_g * whole, parts_g.shape[0]):
        parts_g[i] = jnp.zeros((8, LANES), F32)
    dose = g_ref[...].astype(F32)

    def put(block, parts, first):
        for c in range(block.shape[1] // LANES):
            at = slice(LANES * c, LANES * c + LANES)
            for r in range(whole):
                parts[c * whole + r] = block[8 * r : 8 * r + 8, at]
            for r in range(rest):
                slot, row = spot(first + c, r)
                parts_g[slot, row : row + 1, :] = block[8 * whole + r : 8 * whole + r + 1, at]

    put(jnp.dot(design_t, dose.astype(BF16), preferred_element_type=F32), parts_g, n_t)

    @pl.when(odd == 1)
    def _():
        block = t_ref[:, pl.ds(pl.multiple_of(pair * share, LANES), share)]
        put(jnp.dot(design_t, block, preferred_element_type=F32), parts_t, 0)
        for i in range(n_t * whole, parts_t.shape[0]):
            parts_t[i] = jnp.zeros((8, LANES), F32)

    gram = jnp.dot(design_t, design[...], preferred_element_type=F32)
    gram_part[...] = jnp.zeros(gram_part.shape, F32)
    pack = LANES // (8 * strips)
    for r in range(strips):
        at = slice(r % pack * 8 * strips, (r % pack + 1) * 8 * strips)
        gram_part[r // pack, :, at] = gram[8 * r : 8 * r + 8, : 8 * strips]

    def await_all(sem, like):
        pltpu.make_async_copy(like, like, flat.at[sem]).wait()

    starts = [sum(2 * len(area[0]) for area in areas[:p]) for p in range(n_parts)]

    places = [sum(len(area[0]) for area in areas[:p]) for p in range(n_parts)]

    def source(p, stage):
        return bufs[starts[p] + 2 * stage]

    def target(p, stage):
        return bufs[starts[p] + 2 * stage + 1]

    def digit(p, stage):
        some = areas[p][0][stage]
        return lax.rem(me // 2 ** some[0], 2 ** len(some)), 2 ** len(some), 2 ** some[0]

    def copies(k, p, stage):
        mine, n, far = digit(p, stage)
        at = lax.rem(k, 2), places[p] + stage
        out = []
        for d in range(1, n):
            other = lax.rem(mine + d, n)
            out.append(
                pltpu.make_async_remote_copy(
                    src_ref=source(p, stage).at[k, other],
                    dst_ref=target(p, stage).at[k, d - 1],
                    send_sem=send.at[at],
                    recv_sem=recv.at[at],
                    device_id={"samp": me + (other - mine) * far},
                    device_id_type=MESH,
                )
            )
        return out

    def await_stage(k, p, stage, sems, like):
        sem = sems.at[lax.rem(k, 2), places[p] + stage]
        pltpu.make_async_copy(like, like, sem).wait()

    def await_sent(k, p, stage):
        n = digit(p, stage)[1]
        await_stage(k, p, stage, send, source(p, stage).at[k, pl.ds(0, n - 1)])

    def begin(k, part):
        for p in HALVES[part]:
            for copy in copies(k, p, 0):
                copy.start()

    def advance(k, part, stage, first=False):
        for p in HALVES[part]:
            if stage >= len(areas[p][0]):
                continue
            await_stage(k, p, stage, recv, target(p, stage).at[k])
            if not first:
                await_sent(k - 1, p, stage)
            mine, n, _ = digit(p, stage)
            total = source(p, stage)[k, mine]
            for d in range(1, n):
                total = total + target(p, stage)[k, d - 1]
            if stage < len(areas[p][0]) - 1:
                source(p, stage + 1)[k] = total.reshape(source(p, stage + 1).shape[1:])
                for copy in copies(k, p, stage + 1):
                    copy.start()
            else:
                found[k, areas[p][1], areas[p][2]] = total[0]

    def cross(k, right):
        batch = max(groups // 4, 1)
        for q in range(groups // batch):
            rows = batch * own
            block = jnp.dot(
                rt[q * rows : (q + 1) * rows, :], right, preferred_element_type=F32
            )
            for i in range(batch):
                for p in range(n_parts):
                    order, part_rows, part_lanes = areas[p]
                    lead, other = place_of(order, q * batch + i)
                    source(p, 0)[k, lead, other] = block[i * own : (i + 1) * own][
                        part_rows, part_lanes
                    ]

    pl.semaphore_wait(barrier, 2 * (groups - 1) + tiles - 1)

    def flat_copy(d, source, target, sem, device):
        return pltpu.make_async_remote_copy(
            src_ref=source,
            dst_ref=target,
            send_sem=flat.at[sem],
            recv_sem=flat.at[sem + 1],
            device_id=device,
            device_id_type=MESH,
        )

    def g_copy(d, side, device):
        at = pl.ds(lax.rem(me + d, groups) * quota_g, quota_g)
        return pltpu.make_async_remote_copy(
            src_ref=parts_g.at[at],
            dst_ref=landed_g.at[side, d - 1],
            send_sem=flat.at[2],
            recv_sem=flat.at[3 + side],
            device_id=device,
            device_id_type=MESH,
        )

    @pl.when(odd == 1)
    def _():
        for d in range(1, groups):
            flat_copy(d, gram_part, gram_landed.at[d - 1], 7, samp_peer(d)).start()
        for d in range(1, groups):
            at = pl.ds(lax.rem(me + d, groups) * quota_t, quota_t)
            flat_copy(d, parts_t.at[at], landed_t.at[d - 1], 0, samp_peer(d)).start()
            g_copy(d, 0, samp_peer(d)).start()

    @pl.when(odd == 0)
    def _():
        for d in range(1, groups):
            g_copy(d, 1, {"samp": lax.rem(me + d, groups), "tile": other}).start()
        g_copy(groups, 1, {"tile": other}).start()

    def permute(k, rows):
        order = order_ref[pl.ds(k - 1, 1), :] - me * local
        for i in range(local // step):
            row = lax.broadcasted_iota(jnp.int32, (step, local), 0) + i * step
            hot = jnp.where(row == order, 1.0, 0.0).astype(BF16)
            moved[i * step : (i + 1) * step, : rows.shape[1]] = jnp.dot(
                hot, rows, preferred_element_type=F32
            ).astype(BF16)

    step = min(256, local)
    for i in range(local // step):
        at = slice(i * step, (i + 1) * step)
        rt[:, at] = t_ref[at, :].T
    cross(0, (dose - 1.0).astype(BF16))
    begin(0, 0)
    begin(0, 1)
    permute(1, jnp.concatenate([dose.astype(BF16), design[...]], axis=1))
    swap = pltpu.make_async_remote_copy(
        src_ref=gram_sum,
        dst_ref=gram_sum,
        send_sem=tile_send.at[2 * (tiles - 1)],
        recv_sem=tile_recv.at[2 * (tiles - 1)],
        device_id={"tile": other},
        device_id_type=MESH,
    )

    @pl.when(odd == 1)
    def _():
        await_all(8, gram_landed)
        total = gram_part[...]
        for d in range(1, groups):
            total = total + gram_landed[d - 1]
        gram_sum[...] = total
        swap.start()
        await_all(1, landed_t)
        total = parts_t[pl.ds(me * quota_t, quota_t)]
        for d in range(1, groups):
            total = total + landed_t[d - 1]
        mine[:quota_t] = total
        await_all(3, landed_g.at[0, pl.ds(0, groups - 1)])
        total = parts_g[pl.ds(me * quota_g, quota_g)]
        for d in range(1, groups):
            total = total + landed_g[0, d - 1]
        mine[quota_t : quota_t + quota_g] = total
        await_all(4, landed_g.at[1])
        total = landed_g[1, 0]
        for d in range(1, groups):
            total = total + landed_g[1, d]
        mine[quota_t + quota_g :] = total
        full[pair, me] = mine[...]
        for d in range(1, groups):
            flat_copy(d, mine, full.at[pair, me], 5, samp_peer(d)).start()

    rhs[...] = jnp.zeros(rhs.shape, F32)
    gram_ref[...] = jnp.zeros(gram_ref.shape, F32)
    coef[...] = jnp.zeros(coef.shape, BF16)
    half = LANES // 2

    @pl.when(odd == 0)
    def _():
        swap.wait_recv()

    for r in range(strips):
        at = slice(r % pack * 8 * strips, (r % pack + 1) * 8 * strips)
        gram_ref[8 * r : 8 * r + 8, : 8 * strips] = gram_sum[r // pack][:, at]
    gram = gram_ref[: 8 * strips, :]
    sub = lax.broadcasted_iota(jnp.int32, gram.shape, 0)
    lane = lax.broadcasted_iota(jnp.int32, gram.shape, 1)
    gram = jnp.where(lane == sub + half, 1.0, gram)
    for j in range(used):
        row = gram[j : j + 1, :] * (1.0 / gram[j : j + 1, j : j + 1])
        gram = jnp.where(sub == j, row, gram - gram[:, j : j + 1] * row)
    inverse = jnp.where(lane >= half, gram, 0.0)
    advance(0, 0, 0, True)
    advance(0, 1, 0, True)

    def spread_copy(d, q):
        return pltpu.make_async_remote_copy(
            src_ref=full.at[q],
            dst_ref=full.at[q],
            send_sem=tile_send.at[tiles - 1 + d - 1],
            recv_sem=tile_recv.at[tiles - 1 + q],
            device_id=tile_peer(d),
            device_id_type=MESH,
        )

    @pl.when(odd == 1)
    def _():
        await_all(6, full.at[0, pl.ds(0, groups - 1)])
        for d in range(1, tiles):
            spread_copy(d, pair).start()

    for q in range(pairs):

        @pl.when(jnp.logical_or(odd == 0, pair != q))
        def _():
            spread_copy(1, q).wait_recv()

    for q in range(pairs + 1):
        for c in range(n_t if q < pairs else n_g):
            at = LANES * (q * n_t + c)
            for r in range(whole):
                i = c * whole + r
                if q < pairs:
                    strip = full[q, i // quota_t, i % quota_t]
                else:
                    strip = full[pair, i // quota_g, quota_t + (1 - odd) * quota_g + i % quota_g]
                rhs[half + 8 * r : half + 8 * r + 8, at : at + LANES] = strip
            for r in range(rest):
                i, row = spot(c if q < pairs else n_t + c, r)
                to = half + 8 * whole + r
                if q < pairs:
                    strip = full[q, i // quota_g, quota_t + i % quota_g]
                else:
                    strip = full[pair, i // quota_g, quota_t + (1 - odd) * quota_g + i % quota_g]
                rhs[to : to + 1, at : at + LANES] = strip[row : row + 1, :]
    coef[: 8 * strips, :] = jnp.dot(
        inverse, rhs[...], precision=HIGHEST, preferred_element_type=F32
    ).astype(BF16)

    advance(0, 0, 1, True)
    advance(0, 1, 1, True)
    sq_t = jnp.zeros((1, traits), F32)
    for i in range(local // step):
        at = slice(i * step, (i + 1) * step)
        resid = t_ref[at, :].astype(F32) - jnp.dot(
            design[at, :], coef[:, :traits], preferred_element_type=F32
        )
        sq_t = sq_t + jnp.sum(resid * resid, axis=0, keepdims=True)
        rt[:, at] = resid.astype(BF16).T
    resid = moved[:, :width].astype(F32) - jnp.dot(
        moved[:, width:], coef[:, traits:], preferred_element_type=F32
    )
    cross(1, resid.astype(BF16))
    begin(1, 0)
    begin(1, 1)
    sq_g = jnp.zeros((1, width), F32)
    for i in range(local // step):
        at = slice(i * step, (i + 1) * step)
        resid = g_ref[at, :].astype(F32) - jnp.dot(
            design[at, :], coef[:, traits:], preferred_element_type=F32
        )
        sq_g = sq_g + jnp.sum(resid * resid, axis=0, keepdims=True)
        rg[at, :] = resid.astype(BF16)

    advance(0, 0, 2, True)
    advance(0, 1, 2, True)

    def note_squares():
        for j in range(groups):
            at = j * own // LANES * LANES
            notes[j, 0:1, :] = sq_t[:, at : at + LANES]
            for c in range(n_g):
                notes[j, 1 + c : 2 + c, :] = sq_g[:, c * LANES : (c + 1) * LANES]
            if n_g < 7:
                notes[j, 1 + n_g :, :] = jnp.zeros((7 - n_g, LANES), F32)

    def square_copy(d):
        return pltpu.make_async_remote_copy(
            src_ref=notes.at[lax.rem(me + d, groups)],
            dst_ref=squares.at[d],
            send_sem=flat.at[9],
            recv_sem=flat.at[10],
            device_id=samp_peer(d),
            device_id_type=MESH,
        )

    note_squares()
    squares[0] = notes[me]
    for d in range(1, groups):
        square_copy(d).start()

    lead = pl.multiple_of(me * own // LANES * LANES, LANES)
    shift = pl.multiple_of(lax.rem(me * own, LANES), 8)

    def correct():
        gram = gram_ref[...]
        lane = lax.broadcasted_iota(jnp.int32, gram.shape, 1)
        gram = jnp.where(lane < half, gram, 0.0)
        coef_g = coef[:, traits:].astype(F32)
        miss = rhs[half:, traits:] - jnp.dot(
            gram, coef_g, precision=HIGHEST, preferred_element_type=F32
        )
        sub = lax.broadcasted_iota(jnp.int32, (half, width), 0)
        fit = coef_g[:half] - jnp.where(sub == used - 1, 1.0, 0.0)
        left = jnp.concatenate(
            [rhs[half:, pl.ds(lead, LANES)], coef[:half, pl.ds(lead, LANES)].astype(F32)], axis=0
        )
        column[...] = left.T
        fix[...] = jnp.dot(
            column[pl.ds(shift, own), :],
            jnp.concatenate([fit, miss], axis=0),
            precision=HIGHEST,
            preferred_element_type=F32,
        )

    correct()

    peaks[0] = jnp.zeros(peaks.shape[1:], F32)

    def scale():
        total = squares[0]
        await_all(10, squares.at[pl.ds(1, groups - 1)])
        for d in range(1, groups):
            total = total + squares[d]
        gain = lax.rsqrt(total / samples + epsilon)
        factor = math.sqrt(samples - used - 1) / samples
        for c in range(n_g):
            gain_g[:, c * LANES : (c + 1) * LANES] = jnp.broadcast_to(
                gain[1 + c : 2 + c, :], (8, LANES)
            )
        column[...] = jnp.broadcast_to(gain.T[:, :1] * factor, column.shape)

    def peak_of(k):
        gain_t = column[pl.ds(shift, own), :]
        peak = jnp.max(jnp.abs(found[k] * gain_g[:1, :]), axis=1, keepdims=True) * gain_t
        pos = lax.broadcasted_iota(jnp.int32, peak.shape, 1)
        peaks[0] = jnp.where(pos == k - 1, peak, peaks[0])

    def turn(t, carry):
        for stage in range(3, bits):

            @pl.when(t == stage - 1)
            def _():
                advance(0, 0, stage, True)
                advance(0, 1, stage, True)

        fresh = jnp.logical_and(t > 1, t < turns)

        @pl.when(fresh)
        def _():
            begin(t, 0)

        @pl.when(t + 1 < turns)
        def _():
            permute(t + 1, rg[...])
            cross(t + 1, moved[:, :width])

        for part in range(2):
            if part == 1:

                @pl.when(fresh)
                def _():
                    begin(t, 1)

            for stage in range(bits):
                back = part - 1 - stage
                k = t + back // 2

                @pl.when(jnp.logical_and(k > 0, k < turns))
                def _():
                    advance(k, back % 2, stage)

        @pl.when(t == 2)
        def _():
            scale()

        k = t - (bits + 1) // 2

        @pl.when(k == 0)
        def _():
            score_ref[...] = (
                (found[0] - fix[...]) * gain_g[:1, :] * column[pl.ds(shift, own), :][:, :1]
            )

        @pl.when(k > 0)
        def _():
            peak_of(k)

        return carry

    lax.fori_loop(1, turns + (bits + 1) // 2, turn, 0)
    crossed = [
        pltpu.make_async_remote_copy(
            src_ref=peaks.at[0],
            dst_ref=peaks.at[d],
            send_sem=tile_send.at[d - 1],
            recv_sem=tile_recv.at[d - 1],
            device_id=tile_peer(d),
            device_id_type=MESH,
        )
        for d in range(1, tiles)
    ]
    for copy in crossed:
        copy.start()

    @pl.when(odd == 1)
    def _():
        for d in range(1, tiles):
            spread_copy(d, pair).wait_send()
        swap.wait_send()
        await_all(0, landed_t)
        await_all(2, landed_g.at[0, pl.ds(0, groups - 1)])
        await_all(5, full.at[0, pl.ds(0, groups - 1)])
        await_all(7, gram_landed)

    @pl.when(odd == 0)
    def _():
        await_all(2, landed_g.at[1])

    await_all(9, squares.at[pl.ds(1, groups - 1)])
    for p in range(n_parts):
        for stage in range(len(areas[p][0])):
            await_sent(turns - 1, p, stage)
    top = peaks[0]
    for d in range(1, tiles):
        crossed[d - 1].wait()
        top = jnp.maximum(top, peaks[d])
    peak_ref[...] = top.T[: turns - 1]


def shards(traits, covariates, genotypes, shuffles):
    groups, tiles = lax.axis_size("samp"), lax.axis_size("tile")
    bits = groups.bit_length() - 1
    turns = shuffles.shape[0] + 1
    local, n_traits = traits.shape
    width = genotypes.shape[1]
    used = covariates.shape[1] + 1
    own = n_traits // groups
    areas = parts_of(bits, own, width)
    bufs = []
    for order, part_rows, part_lanes in areas:
        size = (part_rows.stop - part_rows.start, part_lanes.stop - part_lanes.start)
        lot = groups
        for some in order:
            n = 2 ** len(some)
            lot //= n
            bufs.append(pltpu.VMEM((turns, n, lot) + size, F32))
            bufs.append(pltpu.VMEM((turns, n - 1, lot) + size, F32))
    pairs, whole, rest = tiles // 2, used // 8, used % 8
    n_t, n_g, strips = n_traits // pairs // LANES, width // LANES, -(-used // 8)
    quota_t = -(-n_t * whole // groups)
    quota_g = -(-(n_g * whole + -(-(n_t + n_g) * rest // 8)) // groups)
    quota = quota_t + 2 * quota_g
    lots = -(-strips // (LANES // (8 * strips)))
    vmem = pl.BlockSpec(memory_space=pltpu.VMEM)
    sems = pltpu.SemaphoreType.DMA((2, sum(len(area[0]) for area in areas)))
    pair = pltpu.SemaphoreType.DMA((2 * tiles - 1,))
    return pl.pallas_call(
        functools.partial(scan_kernel, groups, tiles, local * groups, used, areas),
        out_shape=(
            pltpu.VMEM((own, width), F32),
            pltpu.VMEM((turns - 1, own), F32),
        ),
        in_specs=[pl.BlockSpec(memory_space=pl.ANY)] * 4,
        out_specs=(vmem, vmem),
        scratch_shapes=[
            pltpu.VMEM((local, n_traits), BF16),
            pltpu.VMEM((used - 1, local), BF16),
            pltpu.VMEM((local, width), jnp.int32),
            pltpu.VMEM((turns - 1, local), jnp.int32),
            pltpu.SemaphoreType.DMA((10,)),
            pltpu.VMEM((local, LANES), BF16),
            pltpu.VMEM((groups * quota_t, 8, LANES), F32),
            pltpu.VMEM((groups * quota_g, 8, LANES), F32),
            pltpu.VMEM((groups - 1, quota_t, 8, LANES), F32),
            pltpu.VMEM((2, groups, quota_g, 8, LANES), F32),
            pltpu.VMEM((quota, 8, LANES), F32),
            pltpu.VMEM((pairs, groups, quota, 8, LANES), F32),
            pltpu.VMEM((LANES, n_traits + width), F32),
            pltpu.VMEM((LANES, n_traits + width), BF16),
            pltpu.VMEM((n_traits, local), BF16),
            pltpu.VMEM((local, width), BF16),
            pltpu.VMEM((local, width + LANES), BF16),
            pltpu.VMEM((turns, own, width), F32),
            pltpu.VMEM((own, width), F32),
            pltpu.VMEM((lots, 8, LANES), F32),
            pltpu.VMEM((groups - 1, lots, 8, LANES), F32),
            pltpu.VMEM((lots, 8, LANES), F32),
            pltpu.VMEM((LANES // 2, LANES), F32),
            pltpu.VMEM((groups, 8, LANES), F32),
            pltpu.VMEM((groups, 8, LANES), F32),
            pltpu.VMEM((LANES, LANES), F32),
            pltpu.VMEM((8, width), F32),
            pltpu.VMEM((tiles, own, LANES), F32),
            pltpu.SemaphoreType.DMA((11,)),
            pair,
            pair,
            sems,
            sems,
            *bufs,
        ],
        compiler_params=pltpu.CompilerParams(
            collective_id=0, has_side_effects=True, vmem_limit_bytes=60 * 1024 * 1024
        ),
        name="scan",
    )(traits, covariates.T, genotypes, shuffles)


def solution(mesh):
    placed = (P("samp", None), P("samp", None), P("samp", "tile"), P(None, "samp"))
    return jax.shard_map(
        shards,
        mesh=mesh,
        in_specs=placed,
        out_specs=(P("samp", "tile"), P(None, "samp")),
        check_vma=False,
    )
```
